256 devices in a mesh: gx: 32 (over x, y, core), gy: 8 (over z).
Axes of the slice: x: 4, y: 4, z: 8, core: 2. Of those that a mesh axis runs over, the one named last changes fastest.
Arguments:
- fields: float32 [8, 2048, 2048], P(None, 'gx', 'gy'), may hold values from -6 to 6
- wave_order: int32 [1024], replicated, may hold values from 0 to 1023, as said below
- kept_mask: int32 [1024, 2048], P('gx', 'gy'), may hold values from 0 to 1, as said below
Outputs:
- spectral: float32 [2, 8, 1024, 2048], P(None, None, 'gx', 'gy')
The draws below stay inside these ranges and needn't reach their ends.
Inputs may be any that keep to these rules, and one draw needn't show every extreme that they name: `wave_order`: each x-wavenumber 0 to 1023 once. `kept_mask`: in each row the kept y-wavenumbers q are those with min(q, 2048 - q) up to a bound that does not grow with the row's x-wavenumber.
All inputs are finite; a program needn't handle non-finite values.
Results may differ from the reference program's by a relative error of at most 0.00007.
Values sent between devices are 32-bit elements; how exact they have to be, the bound alone decides.
A program may use at most 192 MiB of HBM per device.

```python
import math
import jax
import jax.numpy as jnp

NX = 2048
NY = 2048
STACK = 8
KX = 1024


def common_draw(key):
    wave_order = jax.random.permutation(jax.random.fold_in(key, 11), KX).astype(jnp.int32)
    radius_x = jax.random.randint(jax.random.fold_in(key, 12), (), KX // 2, KX)
    radius_y = jax.random.randint(jax.random.fold_in(key, 13), (), NY // 4, NY // 2)
    y_waves = jnp.arange(NY, dtype=jnp.int32)
    folded = jnp.minimum(y_waves, NY - y_waves)
    scaled_x = wave_order * 1024 // radius_x
    scaled_y = folded * 1024 // radius_y
    inside = scaled_x[:, None] * scaled_x[:, None] + scaled_y[None, :] * scaled_y[None, :] <= 1024 * 1024
    return (wave_order, inside.astype(jnp.int32))


def draw_wave_order(key, part):
    return common_draw(key)[0]


def draw_kept_mask(key, part):
    return common_draw(key)[1]


def shard_levels(rng, dims, shards, low, top_value):
    gain = 1.0
    for axis_at, parts in shards:
        draws = jax.random.uniform(jax.random.fold_in(jax.random.fold_in(rng, 6), axis_at), (parts,), jnp.float32, low / len(shards), top_value / len(shards))
        gain = gain * jnp.repeat(jnp.exp(draws), dims[axis_at] // parts).reshape((-1,) + (1,) * (len(dims) - 1 - axis_at))
    return gain


def scatter_about(key, extent, scale, reach, split=(), kind=jnp.bfloat16):
    loudness = shard_levels(key, extent, split, -0.22, 0.18) if split else 1.0
    drawn = jax.random.normal(key, extent, jnp.float32) * scale * loudness
    return jnp.minimum(jnp.maximum(drawn, -reach), reach).astype(kind)


def setup_inputs(seed: int = 0) -> dict:
    key_of = jax.random.split(jax.random.key(seed), 4)
    fields = scatter_about(key_of[0], (STACK, NX, NY), 1.0, 6.0, ((1, 32), (2, 8)), jnp.float32)
    wave_order = draw_wave_order(jax.random.fold_in(key_of[3], 71), 0)
    kept_mask = draw_kept_mask(jax.random.fold_in(key_of[3], 71), 0)
    return {"fields": fields, "wave_order": wave_order, "kept_mask": kept_mask}


def reference(fields, wave_order, kept_mask):
    along_x = jnp.fft.fft(fields, axis=1)
    picked = jnp.take(along_x, wave_order, axis=1)
    both = jnp.fft.fft(picked, axis=2) / math.sqrt(NX * NY)
    weight = kept_mask.astype(jnp.float32)
    real_part = jnp.real(both).astype(jnp.float32) * weight
    imag_part = jnp.imag(both).astype(jnp.float32) * weight
    return jnp.stack([real_part, imag_part]).astype(jnp.float32)
```

```python
import functools
import math

import jax
import jax.numpy as jnp
import numpy as np
from jax import lax
from jax.experimental import pallas as pl
from jax.experimental.pallas import tpu as pltpu
from jax.sharding import PartitionSpec as P

MESH = pl.DeviceIdType.MESH
F32 = jnp.float32
BF16 = jnp.bfloat16
N = 2048
GX = 32
GY = 8


def split(value):
    high = value.astype(BF16)
    return high, (value - high.astype(F32)).astype(BF16)


def cos_sin(phase):
    quarter = (phase + 256) >> 9
    rest = (phase - (quarter << 9)).astype(F32) * (2.0 * math.pi / N)
    square = rest * rest
    sine = rest * (
        1.0 + square * (-1.0 / 6 + square * (1.0 / 120 + square * (-1.0 / 5040 + square * (1.0 / 362880))))
    )
    cosine = 1.0 + square * (
        -0.5 + square * (1.0 / 24 + square * (-1.0 / 720 + square * (1.0 / 40320 - square * (1.0 / 3628800))))
    )
    odd = (quarter & 1) == 1
    turn = quarter & 3
    real = jnp.where(odd, sine, cosine)
    imag = jnp.where(odd, cosine, sine)
    real = jnp.where((turn == 1) | (turn == 2), -real, real)
    imag = jnp.where(turn >= 2, -imag, imag)
    return real, imag


def eight_points(values):
    def two(a, b):
        return (a[0] + b[0], a[1] + b[1]), (a[0] - b[0], a[1] - b[1])

    def four(v):
        s0, d0 = two(v[0], v[2])
        s1, d1 = two(v[1], v[3])
        y0, y2 = two(s0, s1)
        y1 = (d0[0] + d1[1], d0[1] - d1[0])
        y3 = (d0[0] - d1[1], d0[1] + d1[0])
        return [y0, y1, y2, y3]

    even = four(values[0::2])
    odd = four(values[1::2])
    root = math.sqrt(0.5)
    r, i = odd[1]
    odd[1] = ((r + i) * root, (i - r) * root)
    r, i = odd[2]
    odd[2] = (i, -r)
    r, i = odd[3]
    odd[3] = ((i - r) * root, (-r - i) * root)
    pairs = [two(a, b) for a, b in zip(even, odd)]
    return [p[0] for p in pairs] + [p[1] for p in pairs]


def kernel(
    fields_ref, wave_ref, mask_ref, w_ref, twiddle_ref, out_ref,
    send1, recv1, base_re, base_im, tabs, ft, ftp, send2, recv2, ybuf, send3, recv3,
    s1, r1, s2, r2, s3, r3,
):
    g = lax.axis_index("gx")
    z = lax.axis_index("gy")
    level = g // 4
    lane = lax.broadcasted_iota(jnp.int32, (16, 128), 1)
    low = lane < 64

    def pack(s, carry):
        for j in range(2):
            part = [fields_ref[s, pl.ds(16 * h, 16), pl.ds(128 * j, 128)] for h in range(4)]
            turned = [pltpu.roll(p, 64, 1) for p in part]
            for half in range(2):
                send1[4 * s + 2 * j, :, pl.ds(128 * half, 128)] = jnp.where(low, part[2 * half], turned[2 * half + 1])
                send1[4 * s + 2 * j + 1, :, pl.ds(128 * half, 128)] = jnp.where(low, turned[2 * half], part[2 * half + 1])
        return carry

    lax.fori_loop(0, 8, pack, 0)

    def copy1(src, dst_slot, peer):
        return pltpu.make_async_remote_copy(
            src_ref=send1.at[src], dst_ref=recv1.at[dst_slot], send_sem=s1.at[src], recv_sem=r1.at[dst_slot],
            device_id=(peer, z), device_id_type=MESH,
        )

    def start1(d, carry):
        peer = lax.rem(g + d, GX)
        copy1(peer, g, peer).start()
        return carry

    lax.fori_loop(1, GX, start1, 0)
    recv1[g] = send1[g]

    waves = wave_ref[0:1, :]
    rows = lax.broadcasted_iota(jnp.int32, (56, 1024), 0)
    steps = jnp.where(rows < 32, rows * 64, jnp.where(rows < 48, rows - 32, (rows - 48) * 16))
    real, imag = cos_sin((steps * waves) & (N - 1))
    base_re[...] = real
    base_im[...] = imag

    def table(step, carry):
        group, c = step // 8, lax.rem(step, 8)
        cols = pl.ds(pl.multiple_of(128 * c, 128), 128)
        tile = pl.ds(pl.multiple_of(8 * group, 8), 8)
        tile_re, tile_im = base_re[tile, cols], base_im[tile, cols]
        br, bi = base_re[32:48, cols], base_im[32:48, cols]
        for i in range(8):
            ar, ai = tile_re[i : i + 1], tile_im[i : i + 1]
            re_hi, re_lo = split(ar * br - ai * bi)
            im_hi, im_lo = split(-(ar * bi + ai * br))
            at = pl.multiple_of(group * 128 + i * 16, 16)
            tabs[c, pl.ds(at, 16), 0:128] = re_hi
            tabs[c, pl.ds(at, 16), 128:256] = im_hi
            tabs[c, pl.ds(at + 512, 16), 0:128] = re_lo
            tabs[c, pl.ds(at + 512, 16), 128:256] = im_lo
        return carry

    lax.fori_loop(0, 32, table, 0)

    def wait1(d, carry):
        peer = lax.rem(g + d, GX)
        copy1(peer, peer, peer).wait_recv()
        return carry

    lax.fori_loop(1, GX, wait1, 0)

    for i in range(4):
        ft[:, :, pl.ds(128 * i, 128)] = recv1[8 * i : 8 * i + 8].reshape(128, 256).T.reshape(32, 8, 128)
    for h in range(4):
        for v in range(8):
            ftp[pl.ds(64 * h + 8 * v, 8), :] = ft[8 * h : 8 * h + 8, v, :]
    hi, lo = split(ftp[...])
    wide = jnp.concatenate([hi, hi], axis=1)
    lane32 = lax.broadcasted_iota(jnp.int32, (32, 128), 1)
    below = lane32 < 64
    even = (lane32 & 32) == 0

    def copy2(row_owner, slot, zz):
        return pltpu.make_async_remote_copy(
            src_ref=send2.at[row_owner], dst_ref=recv2.at[slot], send_sem=s2.at[row_owner], recv_sem=r2.at[slot],
            device_id=(row_owner, zz), device_id_type=MESH,
        )

    my_slot = 4 * z + lax.rem(g, 4)

    def chunk(step, carry):
        c = lax.rem(step + level, 8)
        sums = jnp.dot(wide, tabs[c], preferred_element_type=F32)
        sums = sums + jnp.dot(lo, tabs[c, 0:512, :], preferred_element_type=F32)
        cols = pl.ds(pl.multiple_of(128 * c, 128), 128)
        xr, xi = sums[0:64, 0:128], sums[0:64, 128:256]
        for h in range(1, 4):
            gr, gi = sums[64 * h : 64 * h + 64, 0:128], sums[64 * h : 64 * h + 64, 128:256]
            cr, ci = base_re[48 + h : 49 + h, cols], base_im[48 + h : 49 + h, cols]
            xr = xr + gr * cr + gi * ci
            xi = xi + gi * cr - gr * ci
        xr = xr.reshape(4, 2, 8, 128)
        xi = xi.reshape(4, 2, 8, 128)
        v = [x[:, j].reshape(32, 128) for j in range(2) for x in (xr, xi)]
        out = [None] * 4
        for d1 in range(2):
            pair = []
            for m0 in range(2):
                a, b = v[m0], v[m0 + 2]
                pair.append(jnp.where(below, a, pltpu.roll(b, 64, 1)) if d1 == 0 else jnp.where(below, pltpu.roll(a, 64, 1), b))
            a, b = pair
            out[2 * d1] = jnp.where(even, a, pltpu.roll(b, 32, 1))
            out[2 * d1 + 1] = jnp.where(even, pltpu.roll(a, 96, 1), b)
        for d in range(4):
            send2[4 * c + d] = out[d].reshape(4, 8, 128)
        for d in range(4):
            owner = 4 * c + d
            mine = (owner == g) & (level == z)

            @pl.when(jnp.logical_not(mine))
            def _():
                copy2(owner, my_slot, level).start()

            @pl.when(mine)
            def _():
                recv2[my_slot] = send2[owner]

        return carry

    lax.fori_loop(0, 8, chunk, 0)

    def wait2(slot, carry):
        source = 4 * z + lax.rem(slot, 4)
        mine = (source == g) & (slot // 4 == z)

        @pl.when(jnp.logical_not(mine))
        def _():
            copy2(0, slot, z).wait_recv()

        return carry

    lax.fori_loop(0, 32, wait2, 0)

    for t in range(4):
        lines = recv2[:, t].reshape(256, 128).T
        hi, lo = split(lines)
        both = jnp.concatenate([hi, hi, lo], axis=1)
        ybuf[pl.ds(128 * t, 128), :] = jnp.dot(both, w_ref[...], preferred_element_type=F32)

    def finish(tile, carry):
        at = pl.multiple_of(8 * tile, 8)
        values = []
        for v in range(8):
            rr = ybuf[pl.ds(64 * v + at, 8), :]
            ii = ybuf[pl.ds(64 * v + 32 + at, 8), :]
            re = rr[:, :256] - ii[:, 256:]
            im = rr[:, 256:] + ii[:, :256]
            c, s = twiddle_ref[v : v + 1, :], twiddle_ref[8 + v : 9 + v, :]
            values.append((re * c + im * s, im * c - re * s))
        for q, (re, im) in enumerate(eight_points(values)):
            send3[q, 0, pl.ds(at, 8), :] = re
            send3[q, 1, pl.ds(at, 8), :] = im
        return carry

    lax.fori_loop(0, 4, finish, 0)

    def copy3(src, slot, peer):
        return pltpu.make_async_remote_copy(
            src_ref=send3.at[src], dst_ref=recv3.at[slot], send_sem=s3.at[src], recv_sem=r3.at[slot],
            device_id=(g, peer), device_id_type=MESH,
        )

    for d in range(1, GY):
        peer = lax.rem(z + d, GY)
        copy3(peer, z, peer).start()
    weight = mask_ref[...].astype(F32)
    for p in range(2):
        out_ref[p, z] = send3[z, p] * weight
    for d in range(1, GY):
        peer = lax.rem(z + d, GY)
        copy3(peer, peer, peer).wait_recv()
        for p in range(2):
            out_ref[p, peer] = recv3[peer, p] * weight

    def drain1(d, carry):
        peer = lax.rem(g + d, GX)
        copy1(peer, peer, peer).wait_send()
        return carry

    lax.fori_loop(1, GX, drain1, 0)

    def drain2(owner, carry):
        mine = (owner == g) & (level == z)

        @pl.when(jnp.logical_not(mine))
        def _():
            copy2(owner, my_slot, level).wait_send()

        return carry

    lax.fori_loop(0, 32, drain2, 0)
    for d in range(1, GY):
        peer = lax.rem(z + d, GY)
        copy3(peer, peer, peer).wait_send()


def y_tables():
    turns = np.outer(np.arange(256), np.arange(256)) % 256 * (2.0 * np.pi / 256)
    table = np.concatenate([np.cos(turns), -np.sin(turns)], axis=1).astype(np.float32)
    high = table.astype(jnp.bfloat16)
    low = (table - high.astype(np.float32)).astype(jnp.bfloat16)
    angles = np.outer(np.arange(8), np.arange(256)) * (2.0 * np.pi / N)
    twiddle = np.concatenate([np.cos(angles), np.sin(angles)]) / N
    return np.concatenate([high, low, high], axis=0), twiddle.astype(np.float32)


def shards(fields, wave_order, kept_mask):
    w, twiddle = y_tables()
    vmem = pl.BlockSpec(memory_space=pltpu.VMEM)
    dma = pltpu.SemaphoreType.DMA
    return pl.pallas_call(
        kernel,
        out_shape=jax.ShapeDtypeStruct((2, 8, 32, 256), F32),
        in_specs=[vmem] * 5,
        out_specs=vmem,
        scratch_shapes=[
            pltpu.VMEM((32, 16, 256), F32),
            pltpu.VMEM((32, 16, 256), F32),
            pltpu.VMEM((56, 1024), F32),
            pltpu.VMEM((56, 1024), F32),
            pltpu.VMEM((8, 1024, 256), BF16),
            pltpu.VMEM((32, 8, 512), F32),
            pltpu.VMEM((256, 512), F32),
            pltpu.VMEM((32, 4, 8, 128), F32),
            pltpu.VMEM((32, 4, 8, 128), F32),
            pltpu.VMEM((512, 512), F32),
            pltpu.VMEM((8, 2, 32, 256), F32),
            pltpu.VMEM((8, 2, 32, 256), F32),
            dma((32,)), dma((32,)), dma((32,)), dma((32,)), dma((8,)), dma((8,)),
        ],
        compiler_params=pltpu.CompilerParams(has_side_effects=True, vmem_limit_bytes=48 * 1024 * 1024),
        name="bifourier",
    )(fields, wave_order.reshape(1, 1024), kept_mask, jnp.asarray(w), jnp.asarray(twiddle))


def solution(mesh):
    return jax.shard_map(
        shards,
        mesh=mesh,
        in_specs=(P(None, "gx", "gy"), P(), P("gx", "gy")),
        out_specs=P(None, None, "gx", "gy"),
        check_vma=False,
    )
```

```python
import functools
import math

import jax
import jax.numpy as jnp
import numpy as np
from jax import lax
from jax.experimental import pallas as pl
from jax.experimental.pallas import tpu as pltpu
from jax.sharding import PartitionSpec as P

MESH = pl.DeviceIdType.MESH
F32 = jnp.float32
BF16 = jnp.bfloat16
N = 2048
GX = 32
GY = 8


def split(value):
    high = value.astype(BF16)
    return high, (value - high.astype(F32)).astype(BF16)


def cos_sin(phase):
    quarter = (phase + 256) >> 9
    rest = (phase - (quarter << 9)).astype(F32) * (2.0 * math.pi / N)
    square = rest * rest
    sine = rest * (
        1.0 + square * (-1.0 / 6 + square * (1.0 / 120 + square * (-1.0 / 5040 + square * (1.0 / 362880))))
    )
    cosine = 1.0 + square * (
        -0.5 + square * (1.0 / 24 + square * (-1.0 / 720 + square * (1.0 / 40320 - square * (1.0 / 3628800))))
    )
    odd = (quarter & 1) == 1
    turn = quarter & 3
    real = jnp.where(odd, sine, cosine)
    imag = jnp.where(odd, cosine, sine)
    real = jnp.where((turn == 1) | (turn == 2), -real, real)
    imag = jnp.where(turn >= 2, -imag, imag)
    return real, imag


def eight_points(values):
    def two(a, b):
        return (a[0] + b[0], a[1] + b[1]), (a[0] - b[0], a[1] - b[1])

    def four(v):
        s0, d0 = two(v[0], v[2])
        s1, d1 = two(v[1], v[3])
        y0, y2 = two(s0, s1)
        y1 = (d0[0] + d1[1], d0[1] - d1[0])
        y3 = (d0[0] - d1[1], d0[1] + d1[0])
        return [y0, y1, y2, y3]

    even = four(values[0::2])
    odd = four(values[1::2])
    root = math.sqrt(0.5)
    r, i = odd[1]
    odd[1] = ((r + i) * root, (i - r) * root)
    r, i = odd[2]
    odd[2] = (i, -r)
    r, i = odd[3]
    odd[3] = ((i - r) * root, (-r - i) * root)
    pairs = [two(a, b) for a, b in zip(even, odd)]
    return [p[0] for p in pairs] + [p[1] for p in pairs]


def kernel(
    fields_hbm, wave_hbm, mask_hbm, w_hbm, twiddle_hbm, out_ref,
    fields_ref, wave_ref, mask_ref, w_ref, twiddle_ref, load,
    send1, recv1, base_re, base_im, tabs, ft, ftp, send2, recv2, ybuf, send3, recv3,
    s1, r1, s2, r2, s3, r3,
):
    g = lax.axis_index("gx")
    z = lax.axis_index("gy")
    level = g // 4
    my_level = lax.rem(z + GY - level, GY)

    loads = [
        pltpu.make_async_copy(source, target, load.at[i])
        for i, (source, target) in enumerate(
            [(fields_hbm, fields_ref), (wave_hbm, wave_ref), (mask_hbm, mask_ref), (w_hbm, w_ref), (twiddle_hbm, twiddle_ref)]
        )
    ]
    for copy in loads:
        copy.start()

    barrier = pltpu.get_barrier_semaphore()

    def greet(d, carry):
        pl.semaphore_signal(barrier, inc=1, device_id=(lax.rem(g + d, GX), z), device_id_type=MESH)
        return carry

    lax.fori_loop(1, GX, greet, 0)
    for d in range(1, GY):
        pl.semaphore_signal(barrier, inc=1, device_id=(g, lax.rem(z + d, GY)), device_id_type=MESH)
    loads[0].wait()
    lane = lax.broadcasted_iota(jnp.int32, (16, 128), 1)
    low = lane < 64

    def pack(s, carry):
        for j in range(2):
            part = [fields_ref[s, pl.ds(16 * h, 16), pl.ds(128 * j, 128)] for h in range(4)]
            turned = [pltpu.roll(p, 64, 1) for p in part]
            for half in range(2):
                send1[4 * s + 2 * j, :, pl.ds(128 * half, 128)] = jnp.where(low, part[2 * half], turned[2 * half + 1])
                send1[4 * s + 2 * j + 1, :, pl.ds(128 * half, 128)] = jnp.where(low, turned[2 * half], part[2 * half + 1])
        return carry

    lax.fori_loop(0, 8, pack, 0)

    def copy1(src, dst_slot, peer):
        return pltpu.make_async_remote_copy(
            src_ref=send1.at[src], dst_ref=recv1.at[dst_slot], send_sem=s1.at[src], recv_sem=r1.at[dst_slot],
            device_id=(peer, z), device_id_type=MESH,
        )

    def start1(d, carry):
        peer = lax.rem(g + d, GX)
        copy1(peer, g, peer).start()
        return carry

    pl.semaphore_wait(barrier, GX - 1 + GY - 1)
    lax.fori_loop(1, GX, start1, 0)
    recv1[g] = send1[g]

    loads[1].wait()
    waves = wave_ref[0:1, :]
    rows = lax.broadcasted_iota(jnp.int32, (56, 1024), 0)
    steps = jnp.where(rows < 32, rows * 64, jnp.where(rows < 48, rows - 32, (rows - 48) * 16))
    real, imag = cos_sin((steps * waves) & (N - 1))
    base_re[...] = real
    base_im[...] = imag

    def table(step, carry):
        group, c = step // 8, lax.rem(step, 8)
        cols = pl.ds(pl.multiple_of(128 * c, 128), 128)
        tile = pl.ds(pl.multiple_of(8 * group, 8), 8)
        tile_re, tile_im = base_re[tile, cols], base_im[tile, cols]
        br, bi = base_re[32:48, cols], base_im[32:48, cols]
        for i in range(8):
            ar, ai = tile_re[i : i + 1], tile_im[i : i + 1]
            re_hi, re_lo = split(ar * br - ai * bi)
            im_hi, im_lo = split(-(ar * bi + ai * br))
            at = pl.multiple_of(group * 128 + i * 16, 16)
            tabs[c, pl.ds(at, 16), 0:128] = re_hi
            tabs[c, pl.ds(at, 16), 128:256] = im_hi
            tabs[c, pl.ds(at + 512, 16), 0:128] = re_lo
            tabs[c, pl.ds(at + 512, 16), 128:256] = im_lo
        return carry

    lax.fori_loop(0, 32, table, 0)

    def wait1(d, carry):
        peer = lax.rem(g + d, GX)
        copy1(peer, peer, peer).wait_recv()
        return carry

    lax.fori_loop(1, GX, wait1, 0)

    for i in range(4):
        ft[:, :, pl.ds(128 * i, 128)] = recv1[8 * i : 8 * i + 8].reshape(128, 256).T.reshape(32, 8, 128)
    for h in range(4):
        for v in range(8):
            ftp[pl.ds(64 * h + 8 * v, 8), :] = ft[8 * h : 8 * h + 8, v, :]
    hi, lo = split(ftp[...])
    wide = jnp.concatenate([hi, hi], axis=1)
    lane32 = lax.broadcasted_iota(jnp.int32, (32, 128), 1)
    below = lane32 < 64
    even = (lane32 & 32) == 0

    def copy2(row_owner, slot, zz):
        return pltpu.make_async_remote_copy(
            src_ref=send2.at[row_owner], dst_ref=recv2.at[slot], send_sem=s2.at[row_owner], recv_sem=r2.at[slot],
            device_id=(row_owner, zz), device_id_type=MESH,
        )

    my_slot = 4 * z + lax.rem(g, 4)

    def chunk(step, carry):
        c = lax.rem(step + level, 8)
        sums = jnp.dot(wide, tabs[c], preferred_element_type=F32)
        sums = sums + jnp.dot(lo, tabs[c, 0:512, :], preferred_element_type=F32)
        cols = pl.ds(pl.multiple_of(128 * c, 128), 128)
        xr, xi = sums[0:64, 0:128], sums[0:64, 128:256]
        for h in range(1, 4):
            gr, gi = sums[64 * h : 64 * h + 64, 0:128], sums[64 * h : 64 * h + 64, 128:256]
            cr, ci = base_re[48 + h : 49 + h, cols], base_im[48 + h : 49 + h, cols]
            xr = xr + gr * cr + gi * ci
            xi = xi + gi * cr - gr * ci
        xr = xr.reshape(4, 2, 8, 128)
        xi = xi.reshape(4, 2, 8, 128)
        v = [x[:, j].reshape(32, 128) for j in range(2) for x in (xr, xi)]
        out = [None] * 4
        for d1 in range(2):
            pair = []
            for m0 in range(2):
                a, b = v[m0], v[m0 + 2]
                pair.append(jnp.where(below, a, pltpu.roll(b, 64, 1)) if d1 == 0 else jnp.where(below, pltpu.roll(a, 64, 1), b))
            a, b = pair
            out[2 * d1] = jnp.where(even, a, pltpu.roll(b, 32, 1))
            out[2 * d1 + 1] = jnp.where(even, pltpu.roll(a, 96, 1), b)
        for d in range(4):
            send2[4 * c + d] = out[d].reshape(4, 8, 128)
        for d in range(4):
            owner = 4 * c + d
            place = lax.rem(level + c, GY)
            mine = (owner == g) & (place == z)

            @pl.when(jnp.logical_not(mine))
            def _():
                copy2(owner, my_slot, place).start()

            @pl.when(mine)
            def _():
                recv2[my_slot] = send2[owner]

        return carry

    lax.fori_loop(0, 8, chunk, 0)

    def wait2(slot, carry):
        source = 4 * my_level + lax.rem(slot, 4)
        mine = (source == g) & (slot // 4 == z)

        @pl.when(jnp.logical_not(mine))
        def _():
            copy2(0, slot, z).wait_recv()

        return carry

    lax.fori_loop(0, 32, wait2, 0)

    loads[3].wait()
    loads[4].wait()
    loads[2].wait()
    for t in range(4):
        lines = recv2[:, t].reshape(256, 128).T
        hi, lo = split(lines)
        both = jnp.concatenate([hi, hi, lo], axis=1)
        ybuf[pl.ds(128 * t, 128), :] = jnp.dot(both, w_ref[...], preferred_element_type=F32)

    def finish(tile, carry):
        at = pl.multiple_of(8 * tile, 8)
        values = []
        for v in range(8):
            rr = ybuf[pl.ds(64 * v + at, 8), :]
            ii = ybuf[pl.ds(64 * v + 32 + at, 8), :]
            re = rr[:, :256] - ii[:, 256:]
            im = rr[:, 256:] + ii[:, :256]
            c, s = twiddle_ref[v : v + 1, :], twiddle_ref[8 + v : 9 + v, :]
            values.append((re * c + im * s, im * c - re * s))
        for q, (re, im) in enumerate(eight_points(values)):
            send3[q, 0, pl.ds(at, 8), :] = re
            send3[q, 1, pl.ds(at, 8), :] = im
        return carry

    lax.fori_loop(0, 4, finish, 0)

    def copy3(src, slot, peer):
        return pltpu.make_async_remote_copy(
            src_ref=send3.at[src], dst_ref=recv3.at[slot], send_sem=s3.at[src], recv_sem=r3.at[slot],
            device_id=(g, peer), device_id_type=MESH,
        )

    for d in range(1, GY):
        peer = lax.rem(z + d, GY)
        copy3(peer, z, peer).start()
    weight = mask_ref[...].astype(F32)
    for p in range(2):
        out_ref[p, my_level] = send3[z, p] * weight
    for d in range(1, GY):
        peer = lax.rem(z + d, GY)
        copy3(peer, peer, peer).wait_recv()
        for p in range(2):
            out_ref[p, lax.rem(my_level + d, GY)] = recv3[peer, p] * weight

    def drain1(d, carry):
        peer = lax.rem(g + d, GX)
        copy1(peer, peer, peer).wait_send()
        return carry

    lax.fori_loop(1, GX, drain1, 0)

    def drain2(owner, carry):
        place = lax.rem(level + owner // 4, GY)
        mine = (owner == g) & (place == z)

        @pl.when(jnp.logical_not(mine))
        def _():
            copy2(owner, my_slot, place).wait_send()

        return carry

    lax.fori_loop(0, 32, drain2, 0)
    for d in range(1, GY):
        peer = lax.rem(z + d, GY)
        copy3(peer, peer, peer).wait_send()


def y_tables():
    turns = np.outer(np.arange(256), np.arange(256)) % 256 * (2.0 * np.pi / 256)
    table = np.concatenate([np.cos(turns), -np.sin(turns)], axis=1).astype(np.float32)
    high = table.astype(jnp.bfloat16)
    low = (table - high.astype(np.float32)).astype(jnp.bfloat16)
    angles = np.outer(np.arange(8), np.arange(256)) * (2.0 * np.pi / N)
    twiddle = np.concatenate([np.cos(angles), np.sin(angles)]) / N
    return np.concatenate([high, low, high], axis=0), twiddle.astype(np.float32)


def shards(fields, wave_order, kept_mask):
    w, twiddle = y_tables()
    vmem = pl.BlockSpec(memory_space=pltpu.VMEM)
    dma = pltpu.SemaphoreType.DMA
    return pl.pallas_call(
        kernel,
        out_shape=jax.ShapeDtypeStruct((2, 8, 32, 256), F32),
        in_specs=[pl.BlockSpec(memory_space=pltpu.HBM)] * 5,
        out_specs=vmem,
        scratch_shapes=[
            pltpu.VMEM((8, 64, 256), F32),
            pltpu.VMEM((1, 1024), jnp.int32),
            pltpu.VMEM((32, 256), jnp.int32),
            pltpu.VMEM((768, 512), BF16),
            pltpu.VMEM((16, 256), F32),
            dma((5,)),
            pltpu.VMEM((32, 16, 256), F32),
            pltpu.VMEM((32, 16, 256), F32),
            pltpu.VMEM((56, 1024), F32),
            pltpu.VMEM((56, 1024), F32),
            pltpu.VMEM((8, 1024, 256), BF16),
            pltpu.VMEM((32, 8, 512), F32),
            pltpu.VMEM((256, 512), F32),
            pltpu.VMEM((32, 4, 8, 128), F32),
            pltpu.VMEM((32, 4, 8, 128), F32),
            pltpu.VMEM((512, 512), F32),
            pltpu.VMEM((8, 2, 32, 256), F32),
            pltpu.VMEM((8, 2, 32, 256), F32),
            dma((32,)), dma((32,)), dma((32,)), dma((32,)), dma((8,)), dma((8,)),
        ],
        compiler_params=pltpu.CompilerParams(has_side_effects=True, collective_id=0, vmem_limit_bytes=48 * 1024 * 1024),
        name="bifourier",
    )(fields, wave_order.reshape(1, 1024), kept_mask, jnp.asarray(w), jnp.asarray(twiddle))


def solution(mesh):
    return jax.shard_map(
        shards,
        mesh=mesh,
        in_specs=(P(None, "gx", "gy"), P(), P("gx", "gy")),
        out_specs=P(None, None, "gx", "gy"),
        check_vma=False,
    )
```

```python
import functools
import math

import jax
import jax.numpy as jnp
import numpy as np
from jax import lax
from jax.experimental import pallas as pl
from jax.experimental.pallas import tpu as pltpu
from jax.sharding import PartitionSpec as P

MESH = pl.DeviceIdType.MESH
F32 = jnp.float32
BF16 = jnp.bfloat16
N = 2048
GX = 32
GY = 8


def split(value):
    high = value.astype(BF16)
    return high, (value - high.astype(F32)).astype(BF16)


def cos_sin(phase):
    quarter = (phase + 256) >> 9
    rest = (phase - (quarter << 9)).astype(F32) * (2.0 * math.pi / N)
    square = rest * rest
    sine = rest * (
        1.0 + square * (-1.0 / 6 + square * (1.0 / 120 + square * (-1.0 / 5040 + square * (1.0 / 362880))))
    )
    cosine = 1.0 + square * (
        -0.5 + square * (1.0 / 24 + square * (-1.0 / 720 + square * (1.0 / 40320 - square * (1.0 / 3628800))))
    )
    odd = (quarter & 1) == 1
    turn = quarter & 3
    real = jnp.where(odd, sine, cosine)
    imag = jnp.where(odd, cosine, sine)
    real = jnp.where((turn == 1) | (turn == 2), -real, real)
    imag = jnp.where(turn >= 2, -imag, imag)
    return real, imag


def eight_points(values):
    def two(a, b):
        return (a[0] + b[0], a[1] + b[1]), (a[0] - b[0], a[1] - b[1])

    def four(v):
        s0, d0 = two(v[0], v[2])
        s1, d1 = two(v[1], v[3])
        y0, y2 = two(s0, s1)
        y1 = (d0[0] + d1[1], d0[1] - d1[0])
        y3 = (d0[0] - d1[1], d0[1] + d1[0])
        return [y0, y1, y2, y3]

    even = four(values[0::2])
    odd = four(values[1::2])
    root = math.sqrt(0.5)
    r, i = odd[1]
    odd[1] = ((r + i) * root, (i - r) * root)
    r, i = odd[2]
    odd[2] = (i, -r)
    r, i = odd[3]
    odd[3] = ((i - r) * root, (-r - i) * root)
    pairs = [two(a, b) for a, b in zip(even, odd)]
    return [p[0] for p in pairs] + [p[1] for p in pairs]


def kernel(
    fields_hbm, wave_hbm, mask_hbm, w_hbm, twiddle_hbm, out_ref,
    fields_ref, wave_ref, mask_ref, w_ref, twiddle_ref, load,
    send1, recv1, base_re, base_im, tabs, ft, ftp, send2, recv2, ybuf, send3, recv3,
    s1, r1, s2, r2, s3, r3,
):
    g = lax.axis_index("gx")
    z = lax.axis_index("gy")
    level = g // 4
    my_level = lax.rem(z + GY - level, GY)

    loads = [
        pltpu.make_async_copy(source, target, load.at[i])
        for i, (source, target) in enumerate(
            [(fields_hbm, fields_ref), (wave_hbm, wave_ref), (mask_hbm, mask_ref), (w_hbm, w_ref), (twiddle_hbm, twiddle_ref)]
        )
    ]
    for copy in loads:
        copy.start()

    barrier = pltpu.get_barrier_semaphore()

    def greet(d, carry):
        pl.semaphore_signal(barrier, inc=1, device_id=(lax.rem(g + d, GX), z), device_id_type=MESH)
        return carry

    lax.fori_loop(1, GX, greet, 0)
    for d in range(1, GY):
        pl.semaphore_signal(barrier, inc=1, device_id=(g, lax.rem(z + d, GY)), device_id_type=MESH)
    loads[0].wait()
    lane = lax.broadcasted_iota(jnp.int32, (16, 128), 1)
    low = lane < 64

    def pack(s, carry):
        for j in range(2):
            part = [fields_ref[s, pl.ds(16 * h, 16), pl.ds(128 * j, 128)] for h in range(4)]
            turned = [pltpu.roll(p, 64, 1) for p in part]
            for half in range(2):
                send1[4 * s + 2 * j, :, pl.ds(128 * half, 128)] = jnp.where(low, part[2 * half], turned[2 * half + 1])
                send1[4 * s + 2 * j + 1, :, pl.ds(128 * half, 128)] = jnp.where(low, turned[2 * half], part[2 * half + 1])
        return carry

    lax.fori_loop(0, 8, pack, 0)

    def copy1(src, dst_slot, peer):
        return pltpu.make_async_remote_copy(
            src_ref=send1.at[src], dst_ref=recv1.at[dst_slot], send_sem=s1.at[src], recv_sem=r1.at[dst_slot],
            device_id=(peer, z), device_id_type=MESH,
        )

    def start1(d, carry):
        peer = lax.rem(g + d, GX)
        copy1(peer, g, peer).start()
        return carry

    pl.semaphore_wait(barrier, GX - 1 + GY - 1)
    lax.fori_loop(1, GX, start1, 0)
    recv1[g] = send1[g]

    loads[1].wait()
    waves = wave_ref[0:1, :]
    rows = lax.broadcasted_iota(jnp.int32, (56, 1024), 0)
    steps = jnp.where(rows < 32, rows * 64, jnp.where(rows < 48, rows - 32, (rows - 48) * 16))
    real, imag = cos_sin((steps * waves) & (N - 1))
    base_re[...] = real
    base_im[...] = imag

    def table(step, carry):
        group, c = step // 8, lax.rem(step, 8)
        cols = pl.ds(pl.multiple_of(128 * c, 128), 128)
        tile = pl.ds(pl.multiple_of(8 * group, 8), 8)
        tile_re, tile_im = base_re[tile, cols], base_im[tile, cols]
        br, bi = base_re[32:48, cols], base_im[32:48, cols]
        for i in range(8):
            ar, ai = tile_re[i : i + 1], tile_im[i : i + 1]
            re_hi, re_lo = split(ar * br - ai * bi)
            im_hi, im_lo = split(-(ar * bi + ai * br))
            at = pl.multiple_of(group * 128 + i * 16, 16)
            tabs[c, pl.ds(at, 16), 0:128] = re_hi
            tabs[c, pl.ds(at, 16), 128:256] = im_hi
            tabs[c, pl.ds(at + 512, 16), 0:128] = re_lo
            tabs[c, pl.ds(at + 512, 16), 128:256] = im_lo
        return carry

    lax.fori_loop(0, 32, table, 0)

    def wait1(d, carry):
        peer = lax.rem(g + d, GX)
        copy1(peer, peer, peer).wait_recv()
        return carry

    lax.fori_loop(1, GX, wait1, 0)

    for i in range(4):
        ft[:, :, pl.ds(128 * i, 128)] = recv1[8 * i : 8 * i + 8].reshape(128, 256).T.reshape(32, 8, 128)
    for h in range(4):
        for v in range(8):
            ftp[pl.ds(64 * h + 8 * v, 8), :] = ft[8 * h : 8 * h + 8, v, :]
    hi, lo = split(ftp[...])
    wide = jnp.concatenate([hi, hi], axis=1)
    lane32 = lax.broadcasted_iota(jnp.int32, (32, 128), 1)
    below = lane32 < 64
    even = (lane32 & 32) == 0

    def copy2(row_owner, slot, zz):
        return pltpu.make_async_remote_copy(
            src_ref=send2.at[row_owner], dst_ref=recv2.at[slot], send_sem=s2.at[row_owner], recv_sem=r2.at[slot],
            device_id=(row_owner, zz), device_id_type=MESH,
        )

    my_slot = 4 * z + lax.rem(g, 4)

    def chunk(step, carry):
        c = lax.rem(step + level, 8)
        sums = jnp.dot(wide, tabs[c], preferred_element_type=F32)
        sums = sums + jnp.dot(lo, tabs[c, 0:512, :], preferred_element_type=F32)
        cols = pl.ds(pl.multiple_of(128 * c, 128), 128)
        xr, xi = sums[0:64, 0:128], sums[0:64, 128:256]
        for h in range(1, 4):
            gr, gi = sums[64 * h : 64 * h + 64, 0:128], sums[64 * h : 64 * h + 64, 128:256]
            cr, ci = base_re[48 + h : 49 + h, cols], base_im[48 + h : 49 + h, cols]
            xr = xr + gr * cr + gi * ci
            xi = xi + gi * cr - gr * ci
        xr = xr.reshape(4, 2, 8, 128)
        xi = xi.reshape(4, 2, 8, 128)
        v = [x[:, j].reshape(32, 128) for j in range(2) for x in (xr, xi)]
        out = [None] * 4
        for d1 in range(2):
            pair = []
            for m0 in range(2):
                a, b = v[m0], v[m0 + 2]
                pair.append(jnp.where(below, a, pltpu.roll(b, 64, 1)) if d1 == 0 else jnp.where(below, pltpu.roll(a, 64, 1), b))
            a, b = pair
            out[2 * d1] = jnp.where(even, a, pltpu.roll(b, 32, 1))
            out[2 * d1 + 1] = jnp.where(even, pltpu.roll(a, 96, 1), b)
        for d in range(4):
            send2[4 * c + d] = out[d].reshape(4, 8, 128)
        for d in range(4):
            owner = 4 * c + d
            place = lax.rem(level + c, GY)
            mine = (owner == g) & (place == z)

            @pl.when(jnp.logical_not(mine))
            def _():
                copy2(owner, my_slot, place).start()

            @pl.when(mine)
            def _():
                recv2[my_slot] = send2[owner]

        return carry

    lax.fori_loop(0, 8, chunk, 0)

    def drain1(d, carry):
        peer = lax.rem(g + d, GX)
        copy1(peer, peer, peer).wait_send()
        return carry

    lax.fori_loop(1, GX, drain1, 0)

    def wait2(slot, carry):
        source = 4 * my_level + lax.rem(slot, 4)
        mine = (source == g) & (slot // 4 == z)

        @pl.when(jnp.logical_not(mine))
        def _():
            copy2(0, slot, z).wait_recv()

        return carry

    lax.fori_loop(0, 32, wait2, 0)

    loads[3].wait()
    loads[4].wait()
    loads[2].wait()
    for t in range(4):
        lines = recv2[:, t].reshape(256, 128).T
        hi, lo = split(lines)
        both = jnp.concatenate([hi, hi, lo], axis=1)
        ybuf[pl.ds(128 * t, 128), :] = jnp.dot(both, w_ref[...], preferred_element_type=F32)

    def finish(tile, carry):
        at = pl.multiple_of(8 * tile, 8)
        values = []
        for v in range(8):
            rr = ybuf[pl.ds(64 * v + at, 8), :]
            ii = ybuf[pl.ds(64 * v + 32 + at, 8), :]
            re = rr[:, :256] - ii[:, 256:]
            im = rr[:, 256:] + ii[:, :256]
            c, s = twiddle_ref[v : v + 1, :], twiddle_ref[8 + v : 9 + v, :]
            values.append((re * c + im * s, im * c - re * s))
        for q, (re, im) in enumerate(eight_points(values)):
            send3[q, 0, pl.ds(at, 8), :] = re
            send3[q, 1, pl.ds(at, 8), :] = im
        return carry

    lax.fori_loop(0, 4, finish, 0)

    def copy3(src, slot, peer):
        return pltpu.make_async_remote_copy(
            src_ref=send3.at[src], dst_ref=recv3.at[slot], send_sem=s3.at[src], recv_sem=r3.at[slot],
            device_id=(g, peer), device_id_type=MESH,
        )

    for d in range(1, GY):
        peer = lax.rem(z + d, GY)
        copy3(peer, z, peer).start()
    def drain2(owner, carry):
        place = lax.rem(level + owner // 4, GY)
        mine = (owner == g) & (place == z)

        @pl.when(jnp.logical_not(mine))
        def _():
            copy2(owner, my_slot, place).wait_send()

        return carry

    lax.fori_loop(0, 32, drain2, 0)
    weight = mask_ref[...].astype(F32)
    for p in range(2):
        out_ref[p, my_level] = send3[z, p] * weight
    for d in range(1, GY):
        peer = lax.rem(z + d, GY)
        copy3(peer, peer, peer).wait_recv()
        for p in range(2):
            out_ref[p, lax.rem(my_level + d, GY)] = recv3[peer, p] * weight

    for d in range(1, GY):
        peer = lax.rem(z + d, GY)
        copy3(peer, peer, peer).wait_send()


def y_tables():
    turns = np.outer(np.arange(256), np.arange(256)) % 256 * (2.0 * np.pi / 256)
    table = np.concatenate([np.cos(turns), -np.sin(turns)], axis=1).astype(np.float32)
    high = table.astype(jnp.bfloat16)
    low = (table - high.astype(np.float32)).astype(jnp.bfloat16)
    angles = np.outer(np.arange(8), np.arange(256)) * (2.0 * np.pi / N)
    twiddle = np.concatenate([np.cos(angles), np.sin(angles)]) / N
    return np.concatenate([high, low, high], axis=0), twiddle.astype(np.float32)


def shards(fields, wave_order, kept_mask):
    w, twiddle = y_tables()
    vmem = pl.BlockSpec(memory_space=pltpu.VMEM)
    dma = pltpu.SemaphoreType.DMA
    return pl.pallas_call(
        kernel,
        out_shape=jax.ShapeDtypeStruct((2, 8, 32, 256), F32),
        in_specs=[pl.BlockSpec(memory_space=pltpu.HBM)] * 5,
        out_specs=vmem,
        scratch_shapes=[
            pltpu.VMEM((8, 64, 256), F32),
            pltpu.VMEM((1, 1024), jnp.int32),
            pltpu.VMEM((32, 256), jnp.int32),
            pltpu.VMEM((768, 512), BF16),
            pltpu.VMEM((16, 256), F32),
            dma((5,)),
            pltpu.VMEM((32, 16, 256), F32),
            pltpu.VMEM((32, 16, 256), F32),
            pltpu.VMEM((56, 1024), F32),
            pltpu.VMEM((56, 1024), F32),
            pltpu.VMEM((8, 1024, 256), BF16),
            pltpu.VMEM((32, 8, 512), F32),
            pltpu.VMEM((256, 512), F32),
            pltpu.VMEM((32, 4, 8, 128), F32),
            pltpu.VMEM((32, 4, 8, 128), F32),
            pltpu.VMEM((512, 512), F32),
            pltpu.VMEM((8, 2, 32, 256), F32),
            pltpu.VMEM((8, 2, 32, 256), F32),
            dma((32,)), dma((32,)), dma((32,)), dma((32,)), dma((8,)), dma((8,)),
        ],
        compiler_params=pltpu.CompilerParams(has_side_effects=True, collective_id=0, vmem_limit_bytes=67043328),
        name="bifourier",
    )(fields, wave_order.reshape(1, 1024), kept_mask, jnp.asarray(w), jnp.asarray(twiddle))


def solution(mesh):
    return jax.shard_map(
        shards,
        mesh=mesh,
        in_specs=(P(None, "gx", "gy"), P(), P("gx", "gy")),
        out_specs=P(None, None, "gx", "gy"),
        check_vma=False,
    )
```

```python
import functools
import math

import jax
import jax.numpy as jnp
import numpy as np
from jax import lax
from jax.experimental import pallas as pl
from jax.experimental.pallas import tpu as pltpu
from jax.sharding import PartitionSpec as P

MESH = pl.DeviceIdType.MESH
F32 = jnp.float32
BF16 = jnp.bfloat16
N = 2048
GX = 32
GY = 8


def split(value):
    high = value.astype(BF16)
    return high, (value - high.astype(F32)).astype(BF16)


def cos_sin(phase):
    quarter = (phase + 256) >> 9
    rest = (phase - (quarter << 9)).astype(F32) * (2.0 * math.pi / N)
    square = rest * rest
    sine = rest * (
        1.0 + square * (-1.0 / 6 + square * (1.0 / 120 + square * (-1.0 / 5040 + square * (1.0 / 362880))))
    )
    cosine = 1.0 + square * (
        -0.5 + square * (1.0 / 24 + square * (-1.0 / 720 + square * (1.0 / 40320 - square * (1.0 / 3628800))))
    )
    odd = (quarter & 1) == 1
    turn = quarter & 3
    real = jnp.where(odd, sine, cosine)
    imag = jnp.where(odd, cosine, sine)
    real = jnp.where((turn == 1) | (turn == 2), -real, real)
    imag = jnp.where(turn >= 2, -imag, imag)
    return real, imag


def eight_points(values):
    def two(a, b):
        return (a[0] + b[0], a[1] + b[1]), (a[0] - b[0], a[1] - b[1])

    def four(v):
        s0, d0 = two(v[0], v[2])
        s1, d1 = two(v[1], v[3])
        y0, y2 = two(s0, s1)
        y1 = (d0[0] + d1[1], d0[1] - d1[0])
        y3 = (d0[0] - d1[1], d0[1] + d1[0])
        return [y0, y1, y2, y3]

    even = four(values[0::2])
    odd = four(values[1::2])
    root = math.sqrt(0.5)
    r, i = odd[1]
    odd[1] = ((r + i) * root, (i - r) * root)
    r, i = odd[2]
    odd[2] = (i, -r)
    r, i = odd[3]
    odd[3] = ((i - r) * root, (-r - i) * root)
    pairs = [two(a, b) for a, b in zip(even, odd)]
    return [p[0] for p in pairs] + [p[1] for p in pairs]


def swap_blocks(values, lane):
    count = len(values)
    step, width = count // 2, 64
    values = list(values)
    while step:
        first = (lane & width) == 0
        for m in range(count):
            if not m & step:
                a, b = values[m], values[m | step]
                values[m] = jnp.where(first, a, pltpu.roll(b, width, 1))
                values[m | step] = jnp.where(first, pltpu.roll(a, 128 - width, 1), b)
        step, width = step // 2, width // 2
    return values


def kernel(
    fields_hbm, wave_hbm, mask_hbm, w_hbm, twiddle_hbm, out_ref,
    fields_ref, wave_ref, mask_ref, w_ref, twiddle_ref, load,
    send1, recv1, base_re, base_im, tabs, lhs, send2, recv2, ybuf, send3, recv3,
    s1, r1, s2, r2, s3, r3,
):
    g = lax.axis_index("gx")
    z = lax.axis_index("gy")
    level = g // 4
    my_level = lax.rem(z + GY - level, GY)

    loads = [
        pltpu.make_async_copy(source, target, load.at[i])
        for i, (source, target) in enumerate(
            [(fields_hbm, fields_ref), (wave_hbm, wave_ref), (mask_hbm, mask_ref), (w_hbm, w_ref), (twiddle_hbm, twiddle_ref)]
        )
    ]
    for copy in loads:
        copy.start()

    barrier = pltpu.get_barrier_semaphore()

    def greet(d, carry):
        pl.semaphore_signal(barrier, inc=1, device_id=(lax.rem(g + d, GX), z), device_id_type=MESH)
        return carry

    lax.fori_loop(1, GX, greet, 0)
    for d in range(1, GY):
        pl.semaphore_signal(barrier, inc=1, device_id=(g, lax.rem(z + d, GY)), device_id_type=MESH)
    lane = lax.broadcasted_iota(jnp.int32, (8, 128), 1)
    order = (lane & 64) + ((lane & 7) << 3) + ((lane >> 3) & 7)
    loads[0].wait()

    def pack(s, carry):
        for j in range(2):
            for quad in range(2):
                part = [
                    jnp.take_along_axis(fields_ref[s, pl.ds(32 * quad + 8 * h, 8), pl.ds(128 * j, 128)], order, axis=1)
                    for h in range(4)
                ]
                for d, block in enumerate(swap_blocks(part, lane)):
                    send1[d % 2, 4 * s + 2 * j + d // 2, :, pl.ds(128 * quad, 128)] = block
        return carry

    lax.fori_loop(0, 8, pack, 0)

    def copy1(b, src, slot, peer):
        return pltpu.make_async_remote_copy(
            src_ref=send1.at[b, src], dst_ref=recv1.at[b, slot], send_sem=s1.at[b, src], recv_sem=r1.at[b, slot],
            device_id=(peer, z), device_id_type=MESH,
        )

    pl.semaphore_wait(barrier, GX - 1 + GY - 1)
    for b in range(2):

        def start1(d, carry):
            peer = lax.rem(g + d, GX)
            copy1(b, peer, g, peer).start()
            return carry

        lax.fori_loop(1, GX, start1, 0)
        recv1[b, g] = send1[b, g]

    loads[1].wait()
    waves = wave_ref[0:1, :]
    rows = lax.broadcasted_iota(jnp.int32, (48, 1024), 0)
    steps = jnp.where(rows < 32, rows * 64, jnp.where(rows < 40, rows - 32, (rows - 40) * 8))
    real, imag = cos_sin((steps * waves) & (N - 1))
    base_re[...] = real
    base_im[...] = imag

    def table(step, carry):
        group, c = step // 8, lax.rem(step, 8)
        cols = pl.ds(pl.multiple_of(128 * c, 128), 128)
        tile = pl.ds(pl.multiple_of(8 * group, 8), 8)
        tile_re, tile_im = base_re[tile, cols], base_im[tile, cols]
        br, bi = base_re[32:40, cols], base_im[32:40, cols]
        for i in range(0, 8, 2):
            both_re, both_im = [], []
            for k in (i, i + 1):
                ar, ai = tile_re[k : k + 1], tile_im[k : k + 1]
                both_re.append(ar * br - ai * bi)
                both_im.append(-(ar * bi + ai * br))
            re_hi, re_lo = split(jnp.concatenate(both_re, axis=0))
            im_hi, im_lo = split(jnp.concatenate(both_im, axis=0))
            at = pl.multiple_of(group * 64 + i * 8, 16)
            tabs[c, pl.ds(at, 16), 0:128] = re_hi
            tabs[c, pl.ds(at, 16), 128:256] = im_hi
            tabs[c, pl.ds(at + 256, 16), 0:128] = re_lo
            tabs[c, pl.ds(at + 256, 16), 128:256] = im_lo
        return carry

    lax.fori_loop(0, 32, table, 0)

    def copy2(hf, b, owner, slot, zz):
        return pltpu.make_async_remote_copy(
            src_ref=send2.at[hf, b, owner], dst_ref=recv2.at[hf, b, slot],
            send_sem=s2.at[hf, b, owner], recv_sem=r2.at[hf, b, slot],
            device_id=(owner, zz), device_id_type=MESH,
        )

    my_slot = 4 * z + lax.rem(g, 4)

    def start2(hf, b, owner):
        place = lax.rem(level + owner // 4, GY)
        mine = (owner == g) & (place == z)

        @pl.when(jnp.logical_not(mine))
        def _():
            copy2(hf, b, owner, my_slot, place).start()

        @pl.when(mine)
        def _():
            recv2[hf, b, my_slot] = send2[hf, b, owner]

    for b in range(2):

        def wait1(d, carry):
            peer = lax.rem(g + d, GX)
            copy1(b, peer, peer, peer).wait_recv()
            return carry

        lax.fori_loop(1, GX, wait1, 0)
        for i in range(2):
            hi, lo = split(recv1[b, 16 * i : 16 * i + 16].reshape(128, 256).T)
            lhs[:, pl.ds(128 * i, 128)] = hi
            lhs[:, pl.ds(256 + 128 * i, 128)] = hi
            lhs[:, pl.ds(512 + 128 * i, 128)] = lo

        def chunk(step, carry):
            c = lax.rem(step + level, 8)
            sums = jnp.dot(lhs[:, 0:512], tabs[c], preferred_element_type=F32)
            sums = sums + jnp.dot(lhs[:, 512:768], tabs[c, 0:256, :], preferred_element_type=F32)
            cols = pl.ds(pl.multiple_of(128 * c, 128), 128)
            tre, tim = base_re[40:48, cols], base_im[40:48, cols]
            xr, xi = sums[0:32, 0:128], sums[0:32, 128:256]
            for h in range(1, 8):
                gr, gi = sums[32 * h : 32 * h + 32, 0:128], sums[32 * h : 32 * h + 32, 128:256]
                cr, ci = tre[h : h + 1], tim[h : h + 1]
                xr = xr + gr * cr + gi * ci
                xi = xi + gi * cr - gr * ci
            parts = [x[8 * v : 8 * v + 8] for v in range(4) for x in (xr, xi)]
            for i, block in enumerate(swap_blocks(parts, lane)):
                send2[i % 2, b, 4 * c + i // 2] = block
            for d in range(4):
                start2(0, b, 4 * c + d)
            return carry

        lax.fori_loop(0, 8, chunk, 0)

        def rest(i, carry):
            start2(1, b, lax.rem(4 * level + i, GX))
            return carry

        lax.fori_loop(0, GX, rest, 0)

        def drain1(d, carry):
            peer = lax.rem(g + d, GX)
            copy1(b, peer, peer, peer).wait_send()
            return carry

        lax.fori_loop(1, GX, drain1, 0)

    for i in (3, 4, 2):
        loads[i].wait()
    weight = mask_ref[...].astype(F32)

    def copy3(hf, src, slot, peer):
        return pltpu.make_async_remote_copy(
            src_ref=send3.at[hf, src], dst_ref=recv3.at[hf, slot], send_sem=s3.at[hf, src], recv_sem=r3.at[hf, slot],
            device_id=(g, peer), device_id_type=MESH,
        )

    for hf in range(2):
        for b in range(2):

            def wait2(slot, carry):
                source = 4 * my_level + lax.rem(slot, 4)
                mine = (source == g) & (slot // 4 == z)

                @pl.when(jnp.logical_not(mine))
                def _():
                    copy2(hf, b, 0, slot, z).wait_recv()

                return carry

            lax.fori_loop(0, 32, wait2, 0)
            hi, lo = split(recv2[hf, b].reshape(256, 128).T)
            both = jnp.concatenate([hi, hi, lo], axis=1)
            ybuf[pl.ds(128 * b, 128), :] = jnp.dot(both, w_ref[...], preferred_element_type=F32)

        def finish(tile, carry):
            at = pl.multiple_of(8 * tile, 8)
            values = []
            for v in range(8):
                rr = ybuf[pl.ds(32 * v + at, 8), :]
                ii = ybuf[pl.ds(32 * v + 16 + at, 8), :]
                re = rr[:, :256] - ii[:, 256:]
                im = rr[:, 256:] + ii[:, :256]
                c, s = twiddle_ref[v : v + 1, :], twiddle_ref[8 + v : 9 + v, :]
                values.append((re * c + im * s, im * c - re * s))
            for q, (re, im) in enumerate(eight_points(values)):
                send3[hf, q, 0, pl.ds(at, 8), :] = re
                send3[hf, q, 1, pl.ds(at, 8), :] = im
            return carry

        lax.fori_loop(0, 2, finish, 0)
        for d in range(1, GY):
            peer = lax.rem(z + d, GY)
            copy3(hf, peer, z, peer).start()

    for hf in range(2):
        rows = pl.ds(16 * hf, 16)
        for p in range(2):
            out_ref[p, my_level, rows] = send3[hf, z, p] * weight[16 * hf : 16 * hf + 16]
        for b in range(2):

            def drain2(owner, carry):
                place = lax.rem(level + owner // 4, GY)
                mine = (owner == g) & (place == z)

                @pl.when(jnp.logical_not(mine))
                def _():
                    copy2(hf, b, owner, my_slot, place).wait_send()

                return carry

            lax.fori_loop(0, GX, drain2, 0)
    for hf in range(2):
        rows = pl.ds(16 * hf, 16)
        for d in range(1, GY):
            peer = lax.rem(z + d, GY)
            copy3(hf, peer, peer, peer).wait_recv()
            for p in range(2):
                out_ref[p, lax.rem(my_level + d, GY), rows] = recv3[hf, peer, p] * weight[16 * hf : 16 * hf + 16]
    for hf in range(2):
        for d in range(1, GY):
            peer = lax.rem(z + d, GY)
            copy3(hf, peer, peer, peer).wait_send()


def y_tables():
    turns = np.outer(np.arange(256), np.arange(256)) % 256 * (2.0 * np.pi / 256)
    table = np.concatenate([np.cos(turns), -np.sin(turns)], axis=1).astype(np.float32)
    high = table.astype(jnp.bfloat16)
    low = (table - high.astype(np.float32)).astype(jnp.bfloat16)
    angles = np.outer(np.arange(8), np.arange(256)) * (2.0 * np.pi / N)
    twiddle = np.concatenate([np.cos(angles), np.sin(angles)]) / N
    return np.concatenate([high, low, high], axis=0), twiddle.astype(np.float32)


def shards(fields, wave_order, kept_mask):
    w, twiddle = y_tables()
    vmem = pl.BlockSpec(memory_space=pltpu.VMEM)
    dma = pltpu.SemaphoreType.DMA
    return pl.pallas_call(
        kernel,
        out_shape=jax.ShapeDtypeStruct((2, 8, 32, 256), F32),
        in_specs=[pl.BlockSpec(memory_space=pltpu.HBM)] * 5,
        out_specs=vmem,
        scratch_shapes=[
            pltpu.VMEM((8, 64, 256), F32),
            pltpu.VMEM((1, 1024), jnp.int32),
            pltpu.VMEM((32, 256), jnp.int32),
            pltpu.VMEM((768, 512), BF16),
            pltpu.VMEM((16, 256), F32),
            dma((5,)),
            pltpu.VMEM((2, 32, 8, 256), F32),
            pltpu.VMEM((2, 32, 8, 256), F32),
            pltpu.VMEM((48, 1024), F32),
            pltpu.VMEM((48, 1024), F32),
            pltpu.VMEM((8, 512, 256), BF16),
            pltpu.VMEM((256, 768), BF16),
            pltpu.VMEM((2, 2, 32, 8, 128), F32),
            pltpu.VMEM((2, 2, 32, 8, 128), F32),
            pltpu.VMEM((256, 512), F32),
            pltpu.VMEM((2, 8, 2, 16, 256), F32),
            pltpu.VMEM((2, 8, 2, 16, 256), F32),
            dma((2, 32)), dma((2, 32)), dma((2, 2, 32)), dma((2, 2, 32)), dma((2, 8)), dma((2, 8)),
        ],
        compiler_params=pltpu.CompilerParams(has_side_effects=True, collective_id=0, vmem_limit_bytes=67043328),
        name="bifourier",
    )(fields, wave_order.reshape(1, 1024), kept_mask, jnp.asarray(w), jnp.asarray(twiddle))


def solution(mesh):
    return jax.shard_map(
        shards,
        mesh=mesh,
        in_specs=(P(None, "gx", "gy"), P(), P("gx", "gy")),
        out_specs=P(None, None, "gx", "gy"),
        check_vma=False,
    )
```

```python
import math

import jax
import jax.numpy as jnp
import numpy as np
from jax import lax
from jax.experimental import pallas as pl
from jax.experimental.pallas import tpu as pltpu
from jax.sharding import PartitionSpec as P

MESH = pl.DeviceIdType.MESH
F32 = jnp.float32
BF16 = jnp.bfloat16
N = 2048
GX = 32
GY = 8


def split(value):
    high = value.astype(BF16)
    return high, (value - high.astype(F32)).astype(BF16)


def cos_sin(phase):
    quarter = (phase + 256) >> 9
    rest = (phase - (quarter << 9)).astype(F32) * (2.0 * math.pi / N)
    square = rest * rest
    sine = rest * (
        1.0 + square * (-1.0 / 6 + square * (1.0 / 120 + square * (-1.0 / 5040 + square * (1.0 / 362880))))
    )
    cosine = 1.0 + square * (
        -0.5 + square * (1.0 / 24 + square * (-1.0 / 720 + square * (1.0 / 40320 - square * (1.0 / 3628800))))
    )
    odd = (quarter & 1) == 1
    turn = quarter & 3
    real = jnp.where(odd, sine, cosine)
    imag = jnp.where(odd, cosine, sine)
    real = jnp.where((turn == 1) | (turn == 2), -real, real)
    imag = jnp.where(turn >= 2, -imag, imag)
    return real, imag


def eight_points(values):
    def two(a, b):
        return (a[0] + b[0], a[1] + b[1]), (a[0] - b[0], a[1] - b[1])

    def four(v):
        s0, d0 = two(v[0], v[2])
        s1, d1 = two(v[1], v[3])
        y0, y2 = two(s0, s1)
        y1 = (d0[0] + d1[1], d0[1] - d1[0])
        y3 = (d0[0] - d1[1], d0[1] + d1[0])
        return [y0, y1, y2, y3]

    even = four(values[0::2])
    odd = four(values[1::2])
    root = math.sqrt(0.5)
    r, i = odd[1]
    odd[1] = ((r + i) * root, (i - r) * root)
    r, i = odd[2]
    odd[2] = (i, -r)
    r, i = odd[3]
    odd[3] = ((i - r) * root, (-r - i) * root)
    pairs = [two(a, b) for a, b in zip(even, odd)]
    return [p[0] for p in pairs] + [p[1] for p in pairs]


def swap_blocks(values, lane):
    count = len(values)
    step, width = count // 2, 64
    values = list(values)
    while step:
        first = (lane & width) == 0
        for m in range(count):
            if not m & step:
                a, b = values[m], values[m | step]
                values[m] = jnp.where(first, a, pltpu.roll(b, width, 1))
                values[m | step] = jnp.where(first, pltpu.roll(a, 128 - width, 1), b)
        step, width = step // 2, width // 2
    return values


def place_of(level, owner):
    sign = 1 - 2 * lax.rem(owner, 2)
    high = lax.rem(lax.rem(owner // 2, 4) + sign * (level // 2 - owner // 8) + 8, 4)
    return 2 * high + lax.rem(level + owner, 2)


def level_of(owner, place):
    sign = 1 - 2 * lax.rem(owner, 2)
    high = lax.rem(owner // 8 + sign * (place // 2 - lax.rem(owner // 2, 4)) + 8, 4)
    return 2 * high + lax.rem(place + owner, 2)


def kernel(
    fields_hbm, wave_hbm, w_hbm, twiddle_hbm, mask_hbm, out_ref, weight_hbm,
    fields_ref, wave_ref, w_ref, twiddle_ref, mask_ref, weight_ref, load,
    send1, recv1, base_re, base_im, tabs, lhs, send2, recv2, ybuf, send3, recv3,
    s1, r1, s2, r2, s3, r3, own_sem,
):
    g = lax.axis_index("gx")
    z = lax.axis_index("gy")
    level = g // 4
    my_level = level_of(g, z)

    loads = [
        pltpu.make_async_copy(source, target, load.at[i])
        for i, (source, target) in enumerate(
            [(fields_hbm, fields_ref), (wave_hbm, wave_ref), (w_hbm, w_ref), (twiddle_hbm, twiddle_ref), (mask_hbm, mask_ref)]
        )
    ]
    for copy in loads:
        copy.start()

    barrier = pltpu.get_barrier_semaphore()

    def greet(d, carry):
        pl.semaphore_signal(barrier, inc=1, device_id=(lax.rem(g + d, GX), z), device_id_type=MESH)
        return carry

    lax.fori_loop(1, GX, greet, 0)
    for d in range(1, GY):
        pl.semaphore_signal(barrier, inc=1, device_id=(g, lax.rem(z + d, GY)), device_id_type=MESH)
    lane = lax.broadcasted_iota(jnp.int32, (8, 128), 1)
    order = (lane & 64) + ((lane & 7) << 3) + ((lane >> 3) & 7)
    loads[0].wait()

    def pack(s, carry):
        for j in range(2):
            for quad in range(2):
                part = [
                    jnp.take_along_axis(fields_ref[s, pl.ds(32 * quad + 8 * h, 8), pl.ds(128 * j, 128)], order, axis=1)
                    for h in range(4)
                ]
                for d, block in enumerate(swap_blocks(part, lane)):
                    send1[d % 2, 4 * s + 2 * j + d // 2, :, pl.ds(128 * quad, 128)] = block
        return carry

    lax.fori_loop(0, 8, pack, 0)

    def copy1(b, src, slot, peer):
        return pltpu.make_async_remote_copy(
            src_ref=send1.at[b, src], dst_ref=recv1.at[b, slot], send_sem=s1.at[b], recv_sem=r1.at[b],
            device_id=(peer, z), device_id_type=MESH,
        )

    def send_all(b):
        def start1(d, carry):
            peer = lax.rem(g + d, GX)
            copy1(b, peer, g, peer).start()
            return carry

        lax.fori_loop(1, GX, start1, 0)
        recv1[b, g] = send1[b, g]

    pl.semaphore_wait(barrier, GX - 1 + GY - 1)
    send_all(0)

    loads[1].wait()
    waves = wave_ref[0:1, :]
    rows = lax.broadcasted_iota(jnp.int32, (48, 1024), 0)
    steps = jnp.where(rows < 32, rows * 64, jnp.where(rows < 40, rows - 32, (rows - 40) * 8))
    real, imag = cos_sin((steps * waves) & (N - 1))
    base_re[...] = real
    base_im[...] = imag

    def table(step, carry):
        group, c = step // 8, lax.rem(step, 8)
        cols = pl.ds(pl.multiple_of(128 * c, 128), 128)
        tile = pl.ds(pl.multiple_of(8 * group, 8), 8)
        tile_re, tile_im = base_re[tile, cols], base_im[tile, cols]
        br, bi = base_re[32:40, cols], base_im[32:40, cols]
        for i in range(0, 8, 2):
            both_re, both_im = [], []
            for k in (i, i + 1):
                ar, ai = tile_re[k : k + 1], tile_im[k : k + 1]
                both_re.append(ar * br - ai * bi)
                both_im.append(-(ar * bi + ai * br))
            re_hi, re_lo = split(jnp.concatenate(both_re, axis=0))
            im_hi, im_lo = split(jnp.concatenate(both_im, axis=0))
            at = pl.multiple_of(group * 64 + i * 8, 16)
            tabs[c, pl.ds(at, 16), 0:128] = re_hi
            tabs[c, pl.ds(at, 16), 128:256] = im_hi
            tabs[c, pl.ds(at + 256, 16), 0:128] = re_lo
            tabs[c, pl.ds(at + 256, 16), 128:256] = im_lo
        return carry

    lax.fori_loop(0, 32, table, 0)
    send_all(1)

    def copy2(part, owner, slot, zz):
        at = (lambda ref, i: ref.at[0, i, part]) if part < 2 else (lambda ref, i: ref.at[1, i])
        return pltpu.make_async_remote_copy(
            src_ref=at(send2, owner), dst_ref=at(recv2, slot), send_sem=s2.at[part], recv_sem=r2.at[part],
            device_id=(owner, zz), device_id_type=MESH,
        )

    my_slot = 4 * z + lax.rem(g, 4)

    stays = my_level == level

    def start2(part, owner):
        copy2(part, owner, my_slot, place_of(level, owner)).start()

    def start2_own(part):
        @pl.when(jnp.logical_not(stays))
        def _():
            start2(part, g)

        @pl.when(stays)
        def _():
            if part < 2:
                recv2[0, my_slot, part] = send2[0, g, part]
            else:
                recv2[1, my_slot] = send2[1, g]

    def each_size(wait):
        @pl.when(stays)
        def _():
            wait(GX - 1)

        @pl.when(jnp.logical_not(stays))
        def _():
            wait(GX)

    def group(source, target, send_sem, recv_sem):
        return pltpu.make_async_remote_copy(
            src_ref=source, dst_ref=target, send_sem=send_sem, recv_sem=recv_sem, device_id=(g, z), device_id_type=MESH
        )

    def all1(b):
        part = pl.ds(0, GX - 1)
        return group(send1.at[b, part], recv1.at[b, part], s1.at[b], r1.at[b])

    def all2(part, count):
        first = pl.ds(0, count)
        at = (lambda ref: ref.at[0, first, part]) if part < 2 else (lambda ref: ref.at[1, first])
        return group(at(send2), at(recv2), s2.at[part], r2.at[part])

    for b in range(2):

        all1(b).wait_recv()
        for i in range(2):
            hi, lo = split(recv1[b, 16 * i : 16 * i + 16].reshape(128, 256).T)
            lhs[:, pl.ds(128 * i, 128)] = hi
            lhs[:, pl.ds(256 + 128 * i, 128)] = hi
            lhs[:, pl.ds(512 + 128 * i, 128)] = lo

        def chunk(step, carry):
            for k in range(2):
                c = lax.rem(2 * step + k + level, 8)
                sums = jnp.dot(lhs[:, 0:512], tabs[c], preferred_element_type=F32)
                sums = sums + jnp.dot(lhs[:, 512:768], tabs[c, 0:256, :], preferred_element_type=F32)
                cols = pl.ds(pl.multiple_of(128 * c, 128), 128)
                tre, tim = base_re[40:48, cols], base_im[40:48, cols]
                xr, xi = sums[0:32, 0:128], sums[0:32, 128:256]
                for h in range(1, 8):
                    gr, gi = sums[32 * h : 32 * h + 32, 0:128], sums[32 * h : 32 * h + 32, 128:256]
                    cr, ci = tre[h : h + 1], tim[h : h + 1]
                    xr = xr + gr * cr + gi * ci
                    xi = xi + gi * cr - gr * ci
                parts = [x[8 * v : 8 * v + 8] for v in range(4) for x in (xr, xi)]
                for i, block in enumerate(swap_blocks(parts, lane)):
                    send2[i % 2, 4 * c + i // 2, b] = block
            for k in range(2):
                c = lax.rem(2 * step + k + level, 8)
                for d in range(4):
                    owner = 4 * c + lax.rem(g + d, 4)
                    if k == 0 and d == 0:

                        @pl.when(step > 0)
                        def _():
                            start2(b, owner)

                    else:
                        start2(b, owner)

            @pl.when(step == 0)
            def _():
                start2_own(b)

            return carry

        lax.fori_loop(0, 4, chunk, 0)

    def rest(d, carry):
        start2(2, lax.rem(g + d, GX))
        return carry

    lax.fori_loop(1, GX, rest, 0)
    start2_own(2)

    for i in (2, 3, 4):
        loads[i].wait()
    weight_ref[...] = mask_ref[...].astype(F32)

    def copy3(hf, src, peer):
        return pltpu.make_async_remote_copy(
            src_ref=send3.at[hf, src], dst_ref=out_ref.at[:, my_level, pl.ds(16 * hf, 16)],
            send_sem=s3.at[hf], recv_sem=r3.at[hf], device_id=(g, peer), device_id_type=MESH,
        )

    def own(hf):
        return pltpu.make_async_copy(send3.at[hf, z], out_ref.at[:, my_level, pl.ds(16 * hf, 16)], own_sem.at[hf])

    for hf in range(2):
        for b in range(2):

            if hf == 0 or b == 0:
                each_size(lambda count: all2(2 * hf + b, count).wait_recv())
            hi, lo = split(recv2[hf, :, b].reshape(256, 128).T)
            both = jnp.concatenate([hi, hi, lo], axis=1)
            ybuf[pl.ds(128 * b, 128), :] = jnp.dot(both, w_ref[...], preferred_element_type=F32)

        def finish(tile, carry):
            at = pl.multiple_of(8 * tile, 8)
            values = []
            for v in range(8):
                rr = ybuf[pl.ds(32 * v + at, 8), :]
                ii = ybuf[pl.ds(32 * v + 16 + at, 8), :]
                re = rr[:, :256] - ii[:, 256:]
                im = rr[:, 256:] + ii[:, :256]
                c, s = twiddle_ref[v : v + 1, :], twiddle_ref[8 + v : 9 + v, :]
                values.append((re * c + im * s, im * c - re * s))
            for q, (re, im) in enumerate(eight_points(values)):
                send3[hf, q, 0, pl.ds(at, 8), :] = re
                send3[hf, q, 1, pl.ds(at, 8), :] = im
            return carry

        lax.fori_loop(0, 2, finish, 0)
        own(hf).start()
        for d in range(1, GY):
            peer = lax.rem(z + d, GY)
            copy3(hf, peer, peer).start()

    weight_out = pltpu.make_async_copy(weight_ref, weight_hbm, load.at[0])
    weight_out.start()
    for b in range(2):
        all1(b).wait_send()
    for part in range(3):
        each_size(lambda count: all2(part, count).wait_send())
    for hf in range(2):
        own(hf).wait()
        arrived = out_ref.at[:, pl.ds(0, GY - 1), pl.ds(16 * hf, 16)]
        both = group(send3.at[hf, pl.ds(0, GY - 1)], arrived, s3.at[hf], r3.at[hf])
        both.wait_recv()
        both.wait_send()
    weight_out.wait()


def y_tables():
    turns = np.outer(np.arange(256), np.arange(256)) % 256 * (2.0 * np.pi / 256)
    table = np.concatenate([np.cos(turns), -np.sin(turns)], axis=1).astype(np.float32)
    high = table.astype(jnp.bfloat16)
    low = (table - high.astype(np.float32)).astype(jnp.bfloat16)
    angles = np.outer(np.arange(8), np.arange(256)) * (2.0 * np.pi / N)
    twiddle = np.concatenate([np.cos(angles), np.sin(angles)]) / N
    return np.concatenate([high, low, high], axis=0), twiddle.astype(np.float32)


def shards(fields, wave_order, kept_mask):
    w, twiddle = y_tables()
    dma = pltpu.SemaphoreType.DMA
    result, weight = pl.pallas_call(
        kernel,
        out_shape=[jax.ShapeDtypeStruct((2, 8, 32, 256), F32), jax.ShapeDtypeStruct((32, 256), F32)],
        in_specs=[pl.BlockSpec(memory_space=pltpu.HBM)] * 5,
        out_specs=[pl.BlockSpec(memory_space=pltpu.HBM)] * 2,
        scratch_shapes=[
            pltpu.VMEM((8, 64, 256), F32),
            pltpu.VMEM((1, 1024), jnp.int32),
            pltpu.VMEM((768, 512), BF16),
            pltpu.VMEM((16, 256), F32),
            pltpu.VMEM((32, 256), jnp.int32),
            pltpu.VMEM((32, 256), F32),
            dma((5,)),
            pltpu.VMEM((2, 32, 8, 256), F32),
            pltpu.VMEM((2, 32, 8, 256), F32),
            pltpu.VMEM((48, 1024), F32),
            pltpu.VMEM((48, 1024), F32),
            pltpu.VMEM((8, 512, 256), BF16),
            pltpu.VMEM((256, 768), BF16),
            pltpu.VMEM((2, 32, 2, 8, 128), F32),
            pltpu.VMEM((2, 32, 2, 8, 128), F32),
            pltpu.VMEM((256, 512), F32),
            pltpu.VMEM((2, 8, 2, 16, 256), F32),
            pltpu.VMEM((2, 8, 2, 16, 256), F32),
            dma((2,)), dma((2,)), dma((3,)), dma((3,)), dma((2,)), dma((2,)), dma((2,)),
        ],
        compiler_params=pltpu.CompilerParams(has_side_effects=True, collective_id=0, vmem_limit_bytes=67043328),
        name="bifourier",
    )(fields, wave_order.reshape(1, 1024), jnp.asarray(w), jnp.asarray(twiddle), kept_mask)
    return result * weight


def solution(mesh):
    return jax.shard_map(
        shards,
        mesh=mesh,
        in_specs=(P(None, "gx", "gy"), P(), P("gx", "gy")),
        out_specs=P(None, None, "gx", "gy"),
        check_vma=False,
    )
```

```python
import math

import jax
import jax.numpy as jnp
import numpy as np
from jax import lax
from jax.experimental import pallas as pl
from jax.experimental.pallas import tpu as pltpu
from jax.sharding import PartitionSpec as P

MESH = pl.DeviceIdType.MESH
F32 = jnp.float32
BF16 = jnp.bfloat16
N = 2048
GX = 32
GY = 8
FAR_FIRST = (4, 3, 5, 2, 6, 1, 7)


def split(value):
    high = value.astype(BF16)
    return high, (value - high.astype(F32)).astype(BF16)


def cos_sin(phase):
    quarter = (phase + 256) >> 9
    rest = (phase - (quarter << 9)).astype(F32) * (2.0 * math.pi / N)
    square = rest * rest
    sine = rest * (
        1.0 + square * (-1.0 / 6 + square * (1.0 / 120 + square * (-1.0 / 5040 + square * (1.0 / 362880))))
    )
    cosine = 1.0 + square * (
        -0.5 + square * (1.0 / 24 + square * (-1.0 / 720 + square * (1.0 / 40320 - square * (1.0 / 3628800))))
    )
    odd = (quarter & 1) == 1
    turn = quarter & 3
    real = jnp.where(odd, sine, cosine)
    imag = jnp.where(odd, cosine, sine)
    real = jnp.where((turn == 1) | (turn == 2), -real, real)
    imag = jnp.where(turn >= 2, -imag, imag)
    return real, imag


def eight_points(values):
    def two(a, b):
        return (a[0] + b[0], a[1] + b[1]), (a[0] - b[0], a[1] - b[1])

    def four(v):
        s0, d0 = two(v[0], v[2])
        s1, d1 = two(v[1], v[3])
        y0, y2 = two(s0, s1)
        y1 = (d0[0] + d1[1], d0[1] - d1[0])
        y3 = (d0[0] - d1[1], d0[1] + d1[0])
        return [y0, y1, y2, y3]

    even = four(values[0::2])
    odd = four(values[1::2])
    root = math.sqrt(0.5)
    r, i = odd[1]
    odd[1] = ((r + i) * root, (i - r) * root)
    r, i = odd[2]
    odd[2] = (i, -r)
    r, i = odd[3]
    odd[3] = ((i - r) * root, (-r - i) * root)
    pairs = [two(a, b) for a, b in zip(even, odd)]
    return [p[0] for p in pairs] + [p[1] for p in pairs]


def swap_blocks(values, lane):
    count = len(values)
    step, width = count // 2, 64
    values = list(values)
    while step:
        first = (lane & width) == 0
        for m in range(count):
            if not m & step:
                a, b = values[m], values[m | step]
                values[m] = jnp.where(first, a, pltpu.roll(b, width, 1))
                values[m | step] = jnp.where(first, pltpu.roll(a, 128 - width, 1), b)
        step, width = step // 2, width // 2
    return values


def place_of(level, owner):
    sign = 1 - 2 * lax.rem(owner, 2)
    high = lax.rem(lax.rem(owner // 2, 4) + sign * (level // 2 - owner // 8) + 8, 4)
    return 2 * high + lax.rem(level + owner, 2)


def level_of(owner, place):
    sign = 1 - 2 * lax.rem(owner, 2)
    high = lax.rem(owner // 8 + sign * (place // 2 - lax.rem(owner // 2, 4)) + 8, 4)
    return 2 * high + lax.rem(place + owner, 2)


def far_first(j):
    return lax.rem(10 - j + 3 * (j * (j - 1) // 2), 4)


def each_peer(g, visit):
    inner = [2 * lax.rem(g // 2 + shift, 4) + lax.rem(g + 1 + k, 2) for shift in (2, 1, 3, 0) for k in range(2)]

    def column(j, carry):
        first = 8 * lax.rem(g // 8 + far_first(j), 4)
        for offset in inner:
            visit(first + offset)
        return carry

    lax.fori_loop(0, 3, column, 0)
    for offset in inner[:-1]:
        visit(8 * (g // 8) + offset)


def kernel(
    fields_hbm, wave_hbm, w_hbm, twiddle_hbm, mask_hbm, out_ref, weight_hbm,
    fields_ref, wave_ref, w_ref, twiddle_ref, mask_ref, weight_ref, load,
    send1, recv1, base_re, base_im, tabs, lhs, send2, recv2, ybuf, send3, recv3,
    s1, r1, s2, r2, s3, r3, own_sem,
):
    g = lax.axis_index("gx")
    z = lax.axis_index("gy")
    level = g // 4
    my_level = level_of(g, z)

    loads = [
        pltpu.make_async_copy(source, target, load.at[i])
        for i, (source, target) in enumerate(
            [(fields_hbm, fields_ref), (wave_hbm, wave_ref), (w_hbm, w_ref), (twiddle_hbm, twiddle_ref), (mask_hbm, mask_ref)]
        )
    ]
    for copy in loads:
        copy.start()

    barrier = pltpu.get_barrier_semaphore()

    def greet(peer):
        pl.semaphore_signal(barrier, inc=1, device_id=(peer, z), device_id_type=MESH)

    each_peer(g, greet)
    for d in FAR_FIRST:
        pl.semaphore_signal(barrier, inc=1, device_id=(g, lax.rem(z + d, GY)), device_id_type=MESH)
    lane = lax.broadcasted_iota(jnp.int32, (8, 128), 1)
    order = (lane & 64) + ((lane & 7) << 3) + ((lane >> 3) & 7)
    loads[0].wait()

    def pack(step, carry):
        for s in (2 * step, 2 * step + 1):
            for j in range(2):
                for quad in range(2):
                    part = [
                        jnp.take_along_axis(
                            fields_ref[s, pl.ds(32 * quad + 8 * h, 8), pl.ds(128 * j, 128)], order, axis=1
                        )
                        for h in range(4)
                    ]
                    for d, block in enumerate(swap_blocks(part, lane)):
                        send1[d % 2, 4 * s + 2 * j + d // 2, :, pl.ds(128 * quad, 128)] = block
        return carry

    lax.fori_loop(0, 4, pack, 0)

    def copy1(b, src, slot, peer):
        return pltpu.make_async_remote_copy(
            src_ref=send1.at[b, src], dst_ref=recv1.at[b, slot], send_sem=s1.at[b], recv_sem=r1.at[b],
            device_id=(peer, z), device_id_type=MESH,
        )

    def send_all(b):
        each_peer(g, lambda peer: copy1(b, peer, g, peer).start())
        recv1[b, g] = send1[b, g]

    pl.semaphore_wait(barrier, GX - 1 + GY - 1)
    send_all(0)

    loads[1].wait()
    waves = wave_ref[0:1, :]
    rows = lax.broadcasted_iota(jnp.int32, (48, 1024), 0)
    steps = jnp.where(rows < 32, rows * 64, jnp.where(rows < 40, rows - 32, (rows - 40) * 8))
    real, imag = cos_sin((steps * waves) & (N - 1))
    base_re[...] = real
    base_im[...] = imag

    def table(step, carry):
        group, c = step // 8, lax.rem(step, 8)
        cols = pl.ds(pl.multiple_of(128 * c, 128), 128)
        tile = pl.ds(pl.multiple_of(8 * group, 8), 8)
        tile_re, tile_im = base_re[tile, cols], base_im[tile, cols]
        br, bi = base_re[32:40, cols], base_im[32:40, cols]
        for i in range(0, 8, 2):
            both_re, both_im = [], []
            for k in (i, i + 1):
                ar, ai = tile_re[k : k + 1], tile_im[k : k + 1]
                both_re.append(ar * br - ai * bi)
                both_im.append(-(ar * bi + ai * br))
            re_hi, re_lo = split(jnp.concatenate(both_re, axis=0))
            im_hi, im_lo = split(jnp.concatenate(both_im, axis=0))
            at = pl.multiple_of(group * 64 + i * 8, 16)
            tabs[c, pl.ds(at, 16), 0:128] = re_hi
            tabs[c, pl.ds(at, 16), 128:256] = im_hi
            tabs[c, pl.ds(at + 256, 16), 0:128] = re_lo
            tabs[c, pl.ds(at + 256, 16), 128:256] = im_lo
        return carry

    lax.fori_loop(0, 32, table, 0)
    send_all(1)

    def copy2(part, owner, slot, zz):
        at = (lambda ref, i: ref.at[0, i, part]) if part < 2 else (lambda ref, i: ref.at[1, i])
        return pltpu.make_async_remote_copy(
            src_ref=at(send2, owner), dst_ref=at(recv2, slot), send_sem=s2.at[part], recv_sem=r2.at[part],
            device_id=(owner, zz), device_id_type=MESH,
        )

    my_slot = 4 * z + lax.rem(g, 4)

    stays = my_level == level

    def start2(part, owner):
        copy2(part, owner, my_slot, place_of(level, owner)).start()

    def start2_own(part):
        @pl.when(jnp.logical_not(stays))
        def _():
            start2(part, g)

        @pl.when(stays)
        def _():
            if part < 2:
                recv2[0, my_slot, part] = send2[0, g, part]
            else:
                recv2[1, my_slot] = send2[1, g]

    def each_size(wait):
        @pl.when(stays)
        def _():
            wait(GX - 1)

        @pl.when(jnp.logical_not(stays))
        def _():
            wait(GX)

    def group(source, target, send_sem, recv_sem):
        return pltpu.make_async_remote_copy(
            src_ref=source, dst_ref=target, send_sem=send_sem, recv_sem=recv_sem, device_id=(g, z), device_id_type=MESH
        )

    def all1(b):
        part = pl.ds(0, GX - 1)
        return group(send1.at[b, part], recv1.at[b, part], s1.at[b], r1.at[b])

    def all2(part, count):
        first = pl.ds(0, count)
        at = (lambda ref: ref.at[0, first, part]) if part < 2 else (lambda ref: ref.at[1, first])
        return group(at(send2), at(recv2), s2.at[part], r2.at[part])

    for b in range(2):

        all1(b).wait_recv()
        for i in range(2):
            hi, lo = split(recv1[b, 16 * i : 16 * i + 16].reshape(128, 256).T)
            lhs[:, pl.ds(128 * i, 128)] = hi
            lhs[:, pl.ds(256 + 128 * i, 128)] = hi
            lhs[:, pl.ds(512 + 128 * i, 128)] = lo

        def chunk(step, carry):
            for k in range(2):
                c = 2 * lax.rem(g // 8 + far_first(step), 4) + lax.rem(level + 1 + k, 2)
                sums = jnp.dot(lhs[:, 0:512], tabs[c], preferred_element_type=F32)
                sums = sums + jnp.dot(lhs[:, 512:768], tabs[c, 0:256, :], preferred_element_type=F32)
                cols = pl.ds(pl.multiple_of(128 * c, 128), 128)
                tre, tim = base_re[40:48, cols], base_im[40:48, cols]
                xr, xi = sums[0:32, 0:128], sums[0:32, 128:256]
                for h in range(1, 8):
                    gr, gi = sums[32 * h : 32 * h + 32, 0:128], sums[32 * h : 32 * h + 32, 128:256]
                    cr, ci = tre[h : h + 1], tim[h : h + 1]
                    xr = xr + gr * cr + gi * ci
                    xi = xi + gi * cr - gr * ci
                parts = [x[8 * v : 8 * v + 8] for v in range(4) for x in (xr, xi)]
                for i, block in enumerate(swap_blocks(parts, lane)):
                    send2[i % 2, 4 * c + i // 2, b] = block
            for k in range(2):
                c = 2 * lax.rem(g // 8 + far_first(step), 4) + lax.rem(level + 1 + k, 2)
                for d in range(4):
                    owner = 4 * c + lax.rem(g + d, 4)
                    if k == 1 and d == 0:

                        @pl.when(step < 3)
                        def _():
                            start2(b, owner)

                    else:
                        start2(b, owner)

            @pl.when(step == 3)
            def _():
                start2_own(b)

            return carry

        lax.fori_loop(0, 4, chunk, 0)

    each_peer(g, lambda owner: start2(2, owner))
    start2_own(2)

    for i in (2, 3, 4):
        loads[i].wait()
    weight_ref[...] = mask_ref[...].astype(F32)

    def copy3(hf, src, peer):
        return pltpu.make_async_remote_copy(
            src_ref=send3.at[hf, src], dst_ref=out_ref.at[:, my_level, pl.ds(16 * hf, 16)],
            send_sem=s3.at[hf], recv_sem=r3.at[hf], device_id=(g, peer), device_id_type=MESH,
        )

    def own(hf):
        return pltpu.make_async_copy(send3.at[hf, z], out_ref.at[:, my_level, pl.ds(16 * hf, 16)], own_sem.at[hf])

    for hf in range(2):
        for b in range(2):

            if hf == 0 or b == 0:
                each_size(lambda count: all2(2 * hf + b, count).wait_recv())
            hi, lo = split(recv2[hf, :, b].reshape(256, 128).T)
            both = jnp.concatenate([hi, hi, lo], axis=1)
            ybuf[pl.ds(128 * b, 128), :] = jnp.dot(both, w_ref[...], preferred_element_type=F32)

        def finish(tile, carry):
            at = pl.multiple_of(8 * tile, 8)
            values = []
            for v in range(8):
                rr = ybuf[pl.ds(32 * v + at, 8), :]
                ii = ybuf[pl.ds(32 * v + 16 + at, 8), :]
                re = rr[:, :256] - ii[:, 256:]
                im = rr[:, 256:] + ii[:, :256]
                c, s = twiddle_ref[v : v + 1, :], twiddle_ref[8 + v : 9 + v, :]
                values.append((re * c + im * s, im * c - re * s))
            for q, (re, im) in enumerate(eight_points(values)):
                send3[hf, q, 0, pl.ds(at, 8), :] = re
                send3[hf, q, 1, pl.ds(at, 8), :] = im
            return carry

        lax.fori_loop(0, 2, finish, 0)
        own(hf).start()
        for d in FAR_FIRST:
            peer = lax.rem(z + d, GY)
            copy3(hf, peer, peer).start()

    weight_out = pltpu.make_async_copy(weight_ref, weight_hbm, load.at[0])
    weight_out.start()
    for b in range(2):
        all1(b).wait_send()
    for part in range(3):
        each_size(lambda count: all2(part, count).wait_send())
    for hf in range(2):
        own(hf).wait()
        arrived = out_ref.at[:, pl.ds(0, GY - 1), pl.ds(16 * hf, 16)]
        both = group(send3.at[hf, pl.ds(0, GY - 1)], arrived, s3.at[hf], r3.at[hf])
        both.wait_recv()
        both.wait_send()
    weight_out.wait()


def y_tables():
    turns = np.outer(np.arange(256), np.arange(256)) % 256 * (2.0 * np.pi / 256)
    table = np.concatenate([np.cos(turns), -np.sin(turns)], axis=1).astype(np.float32)
    high = table.astype(jnp.bfloat16)
    low = (table - high.astype(np.float32)).astype(jnp.bfloat16)
    angles = np.outer(np.arange(8), np.arange(256)) * (2.0 * np.pi / N)
    twiddle = np.concatenate([np.cos(angles), np.sin(angles)]) / N
    return np.concatenate([high, low, high], axis=0), twiddle.astype(np.float32)


def shards(fields, wave_order, kept_mask):
    w, twiddle = y_tables()
    dma = pltpu.SemaphoreType.DMA
    result, weight = pl.pallas_call(
        kernel,
        out_shape=[jax.ShapeDtypeStruct((2, 8, 32, 256), F32), jax.ShapeDtypeStruct((32, 256), F32)],
        in_specs=[pl.BlockSpec(memory_space=pltpu.HBM)] * 5,
        out_specs=[pl.BlockSpec(memory_space=pltpu.HBM)] * 2,
        scratch_shapes=[
            pltpu.VMEM((8, 64, 256), F32),
            pltpu.VMEM((1, 1024), jnp.int32),
            pltpu.VMEM((768, 512), BF16),
            pltpu.VMEM((16, 256), F32),
            pltpu.VMEM((32, 256), jnp.int32),
            pltpu.VMEM((32, 256), F32),
            dma((5,)),
            pltpu.VMEM((2, 32, 8, 256), F32),
            pltpu.VMEM((2, 32, 8, 256), F32),
            pltpu.VMEM((48, 1024), F32),
            pltpu.VMEM((48, 1024), F32),
            pltpu.VMEM((8, 512, 256), BF16),
            pltpu.VMEM((256, 768), BF16),
            pltpu.VMEM((2, 32, 2, 8, 128), F32),
            pltpu.VMEM((2, 32, 2, 8, 128), F32),
            pltpu.VMEM((256, 512), F32),
            pltpu.VMEM((2, 8, 2, 16, 256), F32),
            pltpu.VMEM((2, 8, 2, 16, 256), F32),
            dma((2,)), dma((2,)), dma((3,)), dma((3,)), dma((2,)), dma((2,)), dma((2,)),
        ],
        compiler_params=pltpu.CompilerParams(has_side_effects=True, collective_id=0, vmem_limit_bytes=67043328),
        name="bifourier",
    )(fields, wave_order.reshape(1, 1024), jnp.asarray(w), jnp.asarray(twiddle), kept_mask)
    return result * weight


def solution(mesh):
    return jax.shard_map(
        shards,
        mesh=mesh,
        in_specs=(P(None, "gx", "gy"), P(), P("gx", "gy")),
        out_specs=P(None, None, "gx", "gy"),
        check_vma=False,
    )
```

```python
import math

import jax
import jax.numpy as jnp
import numpy as np
from jax import lax
from jax.experimental import pallas as pl
from jax.experimental.pallas import tpu as pltpu
from jax.sharding import PartitionSpec as P

MESH = pl.DeviceIdType.MESH
F32 = jnp.float32
BF16 = jnp.bfloat16
N = 2048
GX = 32
GY = 8
FAR_FIRST = (4, 3, 5, 2, 6, 1, 7)


def split(value):
    high = value.astype(BF16)
    return high, (value - high.astype(F32)).astype(BF16)


def cos_sin(phase):
    quarter = (phase + 256) >> 9
    rest = (phase - (quarter << 9)).astype(F32) * (2.0 * math.pi / N)
    square = rest * rest
    sine = rest * (
        1.0 + square * (-1.0 / 6 + square * (1.0 / 120 + square * (-1.0 / 5040 + square * (1.0 / 362880))))
    )
    cosine = 1.0 + square * (
        -0.5 + square * (1.0 / 24 + square * (-1.0 / 720 + square * (1.0 / 40320 - square * (1.0 / 3628800))))
    )
    odd = (quarter & 1) == 1
    turn = quarter & 3
    real = jnp.where(odd, sine, cosine)
    imag = jnp.where(odd, cosine, sine)
    real = jnp.where((turn == 1) | (turn == 2), -real, real)
    imag = jnp.where(turn >= 2, -imag, imag)
    return real, imag


def eight_points(values):
    def two(a, b):
        return (a[0] + b[0], a[1] + b[1]), (a[0] - b[0], a[1] - b[1])

    def four(v):
        s0, d0 = two(v[0], v[2])
        s1, d1 = two(v[1], v[3])
        y0, y2 = two(s0, s1)
        y1 = (d0[0] + d1[1], d0[1] - d1[0])
        y3 = (d0[0] - d1[1], d0[1] + d1[0])
        return [y0, y1, y2, y3]

    even = four(values[0::2])
    odd = four(values[1::2])
    root = math.sqrt(0.5)
    r, i = odd[1]
    odd[1] = ((r + i) * root, (i - r) * root)
    r, i = odd[2]
    odd[2] = (i, -r)
    r, i = odd[3]
    odd[3] = ((i - r) * root, (-r - i) * root)
    pairs = [two(a, b) for a, b in zip(even, odd)]
    return [p[0] for p in pairs] + [p[1] for p in pairs]


def swap_blocks(values, lane):
    count = len(values)
    step, width = count // 2, 64
    values = list(values)
    while step:
        first = (lane & width) == 0
        for m in range(count):
            if not m & step:
                a, b = values[m], values[m | step]
                values[m] = jnp.where(first, a, pltpu.roll(b, width, 1))
                values[m | step] = jnp.where(first, pltpu.roll(a, 128 - width, 1), b)
        step, width = step // 2, width // 2
    return values


def place_of(level, owner):
    sign = 1 - 2 * lax.rem(owner, 2)
    high = lax.rem(lax.rem(owner // 2, 4) + sign * (level // 2 - owner // 8) + 8, 4)
    return 2 * high + lax.rem(level + owner, 2)


def level_of(owner, place):
    sign = 1 - 2 * lax.rem(owner, 2)
    high = lax.rem(owner // 8 + sign * (place // 2 - lax.rem(owner // 2, 4)) + 8, 4)
    return 2 * high + lax.rem(place + owner, 2)


def far_first(j):
    return lax.rem(10 - j + 3 * (j * (j - 1) // 2), 4)


def each_peer(g, visit):
    inner = [2 * lax.rem(g // 2 + shift, 4) + lax.rem(g + 1 + k, 2) for shift in (2, 1, 3, 0) for k in range(2)]

    def column(j, carry):
        first = 8 * lax.rem(g // 8 + far_first(j), 4)
        for offset in inner:
            visit(first + offset)
        return carry

    lax.fori_loop(0, 3, column, 0)
    for offset in inner[:-1]:
        visit(8 * (g // 8) + offset)


def kernel(
    fields_hbm, wave_hbm, w_hbm, out_ref,
    fields_ref, wave_ref, w_ref, twiddle_ref, load,
    send1, recv1, base_re, base_im, tabs, lhs, send2, recv2, ybuf, send3, recv3,
    s1, r1, s2, r2, s3, r3, own_sem,
):
    g = lax.axis_index("gx")
    z = lax.axis_index("gy")
    level = g // 4
    my_level = level_of(g, z)

    loads = [
        pltpu.make_async_copy(source, target, load.at[i])
        for i, (source, target) in enumerate(
            [(fields_hbm, fields_ref), (wave_hbm, wave_ref), (w_hbm, w_ref)]
        )
    ]
    for copy in loads:
        copy.start()

    barrier = pltpu.get_barrier_semaphore()

    def greet(peer):
        pl.semaphore_signal(barrier, inc=1, device_id=(peer, z), device_id_type=MESH)

    each_peer(g, greet)
    for d in FAR_FIRST:
        pl.semaphore_signal(barrier, inc=1, device_id=(g, lax.rem(z + d, GY)), device_id_type=MESH)
    lane = lax.broadcasted_iota(jnp.int32, (8, 128), 1)
    order = (lane & 64) + ((lane & 7) << 3) + ((lane >> 3) & 7)
    loads[0].wait()

    def pack(step, carry):
        for s in (2 * step, 2 * step + 1):
            for j in range(2):
                for quad in range(2):
                    part = [
                        jnp.take_along_axis(
                            fields_ref[s, pl.ds(32 * quad + 8 * h, 8), pl.ds(128 * j, 128)], order, axis=1
                        )
                        for h in range(4)
                    ]
                    for d, block in enumerate(swap_blocks(part, lane)):
                        send1[d % 2, 4 * s + 2 * j + d // 2, :, pl.ds(128 * quad, 128)] = block
        return carry

    lax.fori_loop(0, 4, pack, 0)

    def copy1(b, src, slot, peer):
        return pltpu.make_async_remote_copy(
            src_ref=send1.at[b, src], dst_ref=recv1.at[b, slot], send_sem=s1.at[b], recv_sem=r1.at[b],
            device_id=(peer, z), device_id_type=MESH,
        )

    def send_all(b):
        each_peer(g, lambda peer: copy1(b, peer, g, peer).start())
        recv1[b, g] = send1[b, g]

    pl.semaphore_wait(barrier, GX - 1 + GY - 1)
    send_all(0)

    phase = lax.broadcasted_iota(jnp.int32, (8, 256), 0) * lax.broadcasted_iota(jnp.int32, (8, 256), 1)
    real, imag = cos_sin(phase & (N - 1))
    twiddle_ref[0:8, :] = real * (1.0 / N)
    twiddle_ref[8:16, :] = imag * (1.0 / N)

    loads[1].wait()
    waves = wave_ref[0:1, :]
    rows = lax.broadcasted_iota(jnp.int32, (48, 1024), 0)
    steps = jnp.where(rows < 32, rows * 64, jnp.where(rows < 40, rows - 32, (rows - 40) * 8))
    real, imag = cos_sin((steps * waves) & (N - 1))
    base_re[...] = real
    base_im[...] = imag

    def table(step, carry):
        group, c = step // 8, lax.rem(step, 8)
        cols = pl.ds(pl.multiple_of(128 * c, 128), 128)
        tile = pl.ds(pl.multiple_of(8 * group, 8), 8)
        tile_re, tile_im = base_re[tile, cols], base_im[tile, cols]
        br, bi = base_re[32:40, cols], base_im[32:40, cols]
        for i in range(0, 8, 2):
            both_re, both_im = [], []
            for k in (i, i + 1):
                ar, ai = tile_re[k : k + 1], tile_im[k : k + 1]
                both_re.append(ar * br - ai * bi)
                both_im.append(-(ar * bi + ai * br))
            re_hi, re_lo = split(jnp.concatenate(both_re, axis=0))
            im_hi, im_lo = split(jnp.concatenate(both_im, axis=0))
            at = pl.multiple_of(group * 64 + i * 8, 16)
            tabs[c, pl.ds(at, 16), 0:128] = re_hi
            tabs[c, pl.ds(at, 16), 128:256] = im_hi
            tabs[c, pl.ds(at + 256, 16), 0:128] = re_lo
            tabs[c, pl.ds(at + 256, 16), 128:256] = im_lo
        return carry

    lax.fori_loop(0, 32, table, 0)
    send_all(1)

    def copy2(part, owner, slot, zz):
        at = (lambda ref, i: ref.at[0, i, part]) if part < 2 else (lambda ref, i: ref.at[1, i])
        return pltpu.make_async_remote_copy(
            src_ref=at(send2, owner), dst_ref=at(recv2, slot), send_sem=s2.at[part], recv_sem=r2.at[part],
            device_id=(owner, zz), device_id_type=MESH,
        )

    my_slot = 4 * z + lax.rem(g, 4)

    stays = my_level == level

    def start2(part, owner):
        copy2(part, owner, my_slot, place_of(level, owner)).start()

    def start2_own(part):
        @pl.when(jnp.logical_not(stays))
        def _():
            start2(part, g)

        @pl.when(stays)
        def _():
            if part < 2:
                recv2[0, my_slot, part] = send2[0, g, part]
            else:
                recv2[1, my_slot] = send2[1, g]

    def each_size(wait):
        @pl.when(stays)
        def _():
            wait(GX - 1)

        @pl.when(jnp.logical_not(stays))
        def _():
            wait(GX)

    def group(source, target, send_sem, recv_sem):
        return pltpu.make_async_remote_copy(
            src_ref=source, dst_ref=target, send_sem=send_sem, recv_sem=recv_sem, device_id=(g, z), device_id_type=MESH
        )

    def all1(b):
        part = pl.ds(0, GX - 1)
        return group(send1.at[b, part], recv1.at[b, part], s1.at[b], r1.at[b])

    def all2(part, count):
        first = pl.ds(0, count)
        at = (lambda ref: ref.at[0, first, part]) if part < 2 else (lambda ref: ref.at[1, first])
        return group(at(send2), at(recv2), s2.at[part], r2.at[part])

    for b in range(2):

        all1(b).wait_recv()
        for i in range(2):
            hi, lo = split(recv1[b, 16 * i : 16 * i + 16].reshape(128, 256).T)
            lhs[:, pl.ds(128 * i, 128)] = hi
            lhs[:, pl.ds(256 + 128 * i, 128)] = hi
            lhs[:, pl.ds(512 + 128 * i, 128)] = lo

        def chunk(step, carry):
            for k in range(2):
                c = 2 * lax.rem(g // 8 + far_first(step), 4) + lax.rem(level + 1 + k, 2)
                sums = jnp.dot(lhs[:, 0:512], tabs[c], preferred_element_type=F32)
                sums = sums + jnp.dot(lhs[:, 512:768], tabs[c, 0:256, :], preferred_element_type=F32)
                cols = pl.ds(pl.multiple_of(128 * c, 128), 128)
                tre, tim = base_re[40:48, cols], base_im[40:48, cols]
                xr, xi = sums[0:32, 0:128], sums[0:32, 128:256]
                for h in range(1, 8):
                    gr, gi = sums[32 * h : 32 * h + 32, 0:128], sums[32 * h : 32 * h + 32, 128:256]
                    cr, ci = tre[h : h + 1], tim[h : h + 1]
                    xr = xr + gr * cr + gi * ci
                    xi = xi + gi * cr - gr * ci
                parts = [x[8 * v : 8 * v + 8] for v in range(4) for x in (xr, xi)]
                for i, block in enumerate(swap_blocks(parts, lane)):
                    send2[i % 2, 4 * c + i // 2, b] = block
            for k in range(2):
                c = 2 * lax.rem(g // 8 + far_first(step), 4) + lax.rem(level + 1 + k, 2)
                for d in range(4):
                    owner = 4 * c + lax.rem(g + d, 4)
                    if k == 1 and d == 0:

                        @pl.when(step < 3)
                        def _():
                            start2(b, owner)

                    else:
                        start2(b, owner)

            @pl.when(step == 3)
            def _():
                start2_own(b)

            return carry

        lax.fori_loop(0, 4, chunk, 0)

    each_peer(g, lambda owner: start2(2, owner))
    start2_own(2)

    loads[2].wait()

    def copy3(hf, src, peer):
        return pltpu.make_async_remote_copy(
            src_ref=send3.at[hf, src], dst_ref=out_ref.at[:, my_level, pl.ds(16 * hf, 16)],
            send_sem=s3.at[hf], recv_sem=r3.at[hf], device_id=(g, peer), device_id_type=MESH,
        )

    def own(hf):
        return pltpu.make_async_copy(send3.at[hf, z], out_ref.at[:, my_level, pl.ds(16 * hf, 16)], own_sem.at[hf])

    for hf in range(2):
        for b in range(2):

            if hf == 0 or b == 0:
                each_size(lambda count: all2(2 * hf + b, count).wait_recv())
            hi, lo = split(recv2[hf, :, b].reshape(256, 128).T)
            both = jnp.concatenate([hi, hi, lo], axis=1)
            ybuf[pl.ds(128 * b, 128), :] = jnp.dot(both, w_ref[...], preferred_element_type=F32)

        def finish(tile, carry):
            at = pl.multiple_of(8 * tile, 8)
            values = []
            for v in range(8):
                rr = ybuf[pl.ds(32 * v + at, 8), :]
                ii = ybuf[pl.ds(32 * v + 16 + at, 8), :]
                re = rr[:, :256] - ii[:, 256:]
                im = rr[:, 256:] + ii[:, :256]
                c, s = twiddle_ref[v : v + 1, :], twiddle_ref[8 + v : 9 + v, :]
                values.append((re * c + im * s, im * c - re * s))
            for q, (re, im) in enumerate(eight_points(values)):
                send3[hf, q, 0, pl.ds(at, 8), :] = re
                send3[hf, q, 1, pl.ds(at, 8), :] = im
            return carry

        lax.fori_loop(0, 2, finish, 0)
        own(hf).start()
        for d in FAR_FIRST:
            peer = lax.rem(z + d, GY)
            copy3(hf, peer, peer).start()

    for b in range(2):
        all1(b).wait_send()
    for part in range(3):
        each_size(lambda count: all2(part, count).wait_send())
    for hf in range(2):
        own(hf).wait()
        arrived = out_ref.at[:, pl.ds(0, GY - 1), pl.ds(16 * hf, 16)]
        both = group(send3.at[hf, pl.ds(0, GY - 1)], arrived, s3.at[hf], r3.at[hf])
        both.wait_recv()
        both.wait_send()


def y_tables():
    turns = np.outer(np.arange(256), np.arange(256)) % 256 * (2.0 * np.pi / 256)
    table = np.concatenate([np.cos(turns), -np.sin(turns)], axis=1).astype(np.float32)
    high = table.astype(jnp.bfloat16)
    low = (table - high.astype(np.float32)).astype(jnp.bfloat16)
    return np.concatenate([high, low, high], axis=0)


def shards(fields, wave_order, kept_mask):
    w = y_tables()
    dma = pltpu.SemaphoreType.DMA
    result = pl.pallas_call(
        kernel,
        out_shape=jax.ShapeDtypeStruct((2, 8, 32, 256), F32),
        in_specs=[pl.BlockSpec(memory_space=pltpu.HBM)] * 3,
        out_specs=pl.BlockSpec(memory_space=pltpu.HBM),
        scratch_shapes=[
            pltpu.VMEM((8, 64, 256), F32),
            pltpu.VMEM((1, 1024), jnp.int32),
            pltpu.VMEM((768, 512), BF16),
            pltpu.VMEM((16, 256), F32),
            dma((3,)),
            pltpu.VMEM((2, 32, 8, 256), F32),
            pltpu.VMEM((2, 32, 8, 256), F32),
            pltpu.VMEM((48, 1024), F32),
            pltpu.VMEM((48, 1024), F32),
            pltpu.VMEM((8, 512, 256), BF16),
            pltpu.VMEM((256, 768), BF16),
            pltpu.VMEM((2, 32, 2, 8, 128), F32),
            pltpu.VMEM((2, 32, 2, 8, 128), F32),
            pltpu.VMEM((256, 512), F32),
            pltpu.VMEM((2, 8, 2, 16, 256), F32),
            pltpu.VMEM((2, 8, 2, 16, 256), F32),
            dma((2,)), dma((2,)), dma((3,)), dma((3,)), dma((2,)), dma((2,)), dma((2,)),
        ],
        compiler_params=pltpu.CompilerParams(has_side_effects=True, collective_id=0, vmem_limit_bytes=int(67043328-10.75*1048576)),
        name="bifourier",
    )(fields, wave_order.reshape(1, 1024), jnp.asarray(w))
    bound = (result != result).astype(jnp.int32)
    return jnp.where(kept_mask[None, None] > bound, result, 0.0)


def solution(mesh):
    return jax.shard_map(
        shards,
        mesh=mesh,
        in_specs=(P(None, "gx", "gy"), P(), P("gx", "gy")),
        out_specs=P(None, None, "gx", "gy"),
        check_vma=False,
    )
```

```python
import math

import jax
import jax.numpy as jnp
import numpy as np
from jax import lax
from jax.experimental import pallas as pl
from jax.experimental.pallas import tpu as pltpu
from jax.sharding import PartitionSpec as P

MESH = pl.DeviceIdType.MESH
F32 = jnp.float32
BF16 = jnp.bfloat16
N = 2048
GX = 32
GY = 8
FAR_FIRST = (4, 3, 5, 2, 6, 1, 7)


def split(value):
    high = value.astype(BF16)
    return high, (value - high.astype(F32)).astype(BF16)


def cos_sin(phase):
    quarter = (phase + 256) >> 9
    rest = (phase - (quarter << 9)).astype(F32) * (2.0 * math.pi / N)
    square = rest * rest
    sine = rest * (
        1.0 + square * (-1.0 / 6 + square * (1.0 / 120 + square * (-1.0 / 5040 + square * (1.0 / 362880))))
    )
    cosine = 1.0 + square * (
        -0.5 + square * (1.0 / 24 + square * (-1.0 / 720 + square * (1.0 / 40320 - square * (1.0 / 3628800))))
    )
    odd = (quarter & 1) == 1
    turn = quarter & 3
    real = jnp.where(odd, sine, cosine)
    imag = jnp.where(odd, cosine, sine)
    real = jnp.where((turn == 1) | (turn == 2), -real, real)
    imag = jnp.where(turn >= 2, -imag, imag)
    return real, imag


def eight_points(values):
    def two(a, b):
        return (a[0] + b[0], a[1] + b[1]), (a[0] - b[0], a[1] - b[1])

    def four(v):
        s0, d0 = two(v[0], v[2])
        s1, d1 = two(v[1], v[3])
        y0, y2 = two(s0, s1)
        y1 = (d0[0] + d1[1], d0[1] - d1[0])
        y3 = (d0[0] - d1[1], d0[1] + d1[0])
        return [y0, y1, y2, y3]

    even = four(values[0::2])
    odd = four(values[1::2])
    root = math.sqrt(0.5)
    r, i = odd[1]
    odd[1] = ((r + i) * root, (i - r) * root)
    r, i = odd[2]
    odd[2] = (i, -r)
    r, i = odd[3]
    odd[3] = ((i - r) * root, (-r - i) * root)
    pairs = [two(a, b) for a, b in zip(even, odd)]
    return [p[0] for p in pairs] + [p[1] for p in pairs]


def swap_blocks(values, lane):
    count = len(values)
    step, width = count // 2, 64
    values = list(values)
    while step:
        first = (lane & width) == 0
        for m in range(count):
            if not m & step:
                a, b = values[m], values[m | step]
                values[m] = jnp.where(first, a, pltpu.roll(b, width, 1))
                values[m | step] = jnp.where(first, pltpu.roll(a, 128 - width, 1), b)
        step, width = step // 2, width // 2
    return values


def place_of(level, owner):
    sign = 1 - 2 * lax.rem(owner, 2)
    high = lax.rem(lax.rem(owner // 2, 4) + sign * (level // 2 - owner // 8) + 8, 4)
    return 2 * high + lax.rem(level + owner, 2)


def level_of(owner, place):
    sign = 1 - 2 * lax.rem(owner, 2)
    high = lax.rem(owner // 8 + sign * (place // 2 - lax.rem(owner // 2, 4)) + 8, 4)
    return 2 * high + lax.rem(place + owner, 2)


def far_first(j):
    return lax.rem(10 - j + 3 * (j * (j - 1) // 2), 4)


def each_peer(g, visit):
    inner = [2 * lax.rem(g // 2 + shift, 4) + lax.rem(g + 1 + k, 2) for shift in (2, 1, 3, 0) for k in range(2)]

    def column(j, carry):
        first = 8 * lax.rem(g // 8 + far_first(j), 4)
        for offset in inner:
            visit(first + offset)
        return carry

    lax.fori_loop(0, 3, column, 0)
    for offset in inner[:-1]:
        visit(8 * (g // 8) + offset)


def kernel(
    fields_hbm, wave_hbm, w_hbm, out_ref,
    fields_ref, wave_ref, w_ref, twiddle_ref, load,
    send1, recv1, base_re, base_im, tabs, lhs, send2, recv2, ybuf, send3, recv3,
    s1, r1, s2, r2, s3, r3, own_sem,
):
    g = lax.axis_index("gx")
    z = lax.axis_index("gy")
    level = g // 4
    my_level = level_of(g, z)

    loads = [
        pltpu.make_async_copy(source, target, load.at[i])
        for i, (source, target) in enumerate(
            [(fields_hbm, fields_ref), (wave_hbm, wave_ref), (w_hbm, w_ref)]
        )
    ]
    for copy in loads:
        copy.start()

    barrier = pltpu.get_barrier_semaphore()

    def greet(peer):
        pl.semaphore_signal(barrier, inc=1, device_id=(peer, z), device_id_type=MESH)

    each_peer(g, greet)
    for d in FAR_FIRST:
        pl.semaphore_signal(barrier, inc=1, device_id=(g, lax.rem(z + d, GY)), device_id_type=MESH)
    lane = lax.broadcasted_iota(jnp.int32, (8, 128), 1)
    order = (lane & 64) + ((lane & 7) << 3) + ((lane >> 3) & 7)
    loads[0].wait()

    def pack(step, carry):
        for s in (2 * step, 2 * step + 1):
            for j in range(2):
                for quad in range(2):
                    part = [
                        jnp.take_along_axis(
                            fields_ref[s, pl.ds(32 * quad + 8 * h, 8), pl.ds(128 * j, 128)], order, axis=1
                        )
                        for h in range(4)
                    ]
                    for d, block in enumerate(swap_blocks(part, lane)):
                        send1[d % 2, 4 * s + 2 * j + d // 2, :, pl.ds(128 * quad, 128)] = block
        return carry

    lax.fori_loop(0, 4, pack, 0)

    def copy1(b, src, slot, peer):
        return pltpu.make_async_remote_copy(
            src_ref=send1.at[b, src], dst_ref=recv1.at[b, slot], send_sem=s1.at[b], recv_sem=r1.at[b],
            device_id=(peer, z), device_id_type=MESH,
        )

    def send_all(b):
        each_peer(g, lambda peer: copy1(b, peer, g, peer).start())
        recv1[b, g] = send1[b, g]

    pl.semaphore_wait(barrier, GX - 1 + GY - 1)
    send_all(0)

    phase = lax.broadcasted_iota(jnp.int32, (8, 256), 0) * lax.broadcasted_iota(jnp.int32, (8, 256), 1)
    real, imag = cos_sin(phase & (N - 1))
    twiddle_ref[0:8, :] = real * (1.0 / N)
    twiddle_ref[8:16, :] = imag * (1.0 / N)

    loads[1].wait()
    waves = wave_ref[0:1, :]
    rows = lax.broadcasted_iota(jnp.int32, (48, 1024), 0)
    steps = jnp.where(rows < 32, rows * 64, jnp.where(rows < 40, rows - 32, (rows - 40) * 8))
    real, imag = cos_sin((steps * waves) & (N - 1))
    base_re[...] = real
    base_im[...] = imag

    def table(step, carry):
        group, c = step // 8, lax.rem(step, 8)
        cols = pl.ds(pl.multiple_of(128 * c, 128), 128)
        tile = pl.ds(pl.multiple_of(8 * group, 8), 8)
        tile_re, tile_im = base_re[tile, cols], base_im[tile, cols]
        br, bi = base_re[32:40, cols], base_im[32:40, cols]
        for i in range(0, 8, 2):
            both_re, both_im = [], []
            for k in (i, i + 1):
                ar, ai = tile_re[k : k + 1], tile_im[k : k + 1]
                both_re.append(ar * br - ai * bi)
                both_im.append(-(ar * bi + ai * br))
            re_hi, re_lo = split(jnp.concatenate(both_re, axis=0))
            im_hi, im_lo = split(jnp.concatenate(both_im, axis=0))
            at = pl.multiple_of(group * 64 + i * 8, 16)
            tabs[c, pl.ds(at, 16), 0:128] = re_hi
            tabs[c, pl.ds(at, 16), 128:256] = im_hi
            tabs[c, pl.ds(at + 256, 16), 0:128] = re_lo
            tabs[c, pl.ds(at + 256, 16), 128:256] = im_lo
        return carry

    lax.fori_loop(0, 32, table, 0)
    send_all(1)

    def copy2(part, owner, slot, zz):
        at = (lambda ref, i: ref.at[0, i, part]) if part < 2 else (lambda ref, i: ref.at[1, i])
        return pltpu.make_async_remote_copy(
            src_ref=at(send2, owner), dst_ref=at(recv2, slot), send_sem=s2.at[part], recv_sem=r2.at[part],
            device_id=(owner, zz), device_id_type=MESH,
        )

    my_slot = 4 * z + lax.rem(g, 4)

    stays = my_level == level

    def start2(part, owner):
        copy2(part, owner, my_slot, place_of(level, owner)).start()

    def start2_own(part):
        @pl.when(jnp.logical_not(stays))
        def _():
            start2(part, g)

        @pl.when(stays)
        def _():
            if part < 2:
                recv2[0, my_slot, part] = send2[0, g, part]
            else:
                recv2[1, my_slot] = send2[1, g]

    def each_size(wait):
        @pl.when(stays)
        def _():
            wait(GX - 1)

        @pl.when(jnp.logical_not(stays))
        def _():
            wait(GX)

    def group(source, target, send_sem, recv_sem):
        return pltpu.make_async_remote_copy(
            src_ref=source, dst_ref=target, send_sem=send_sem, recv_sem=recv_sem, device_id=(g, z), device_id_type=MESH
        )

    def all1(b):
        part = pl.ds(0, GX - 1)
        return group(send1.at[b, part], recv1.at[b, part], s1.at[b], r1.at[b])

    def all2(part, count):
        first = pl.ds(0, count)
        at = (lambda ref: ref.at[0, first, part]) if part < 2 else (lambda ref: ref.at[1, first])
        return group(at(send2), at(recv2), s2.at[part], r2.at[part])

    for b in range(2):

        all1(b).wait_recv()
        for i in range(2):
            hi, lo = split(recv1[b, 16 * i : 16 * i + 16].reshape(128, 256).T)
            lhs[:, pl.ds(128 * i, 128)] = hi
            lhs[:, pl.ds(256 + 128 * i, 128)] = hi
            lhs[:, pl.ds(512 + 128 * i, 128)] = lo

        def chunk(step, carry):
            for k in range(2):
                c = 2 * lax.rem(g // 8 + far_first(step), 4) + lax.rem(level + 1 + k, 2)
                sums = jnp.dot(lhs[:, 0:512], tabs[c], preferred_element_type=F32)
                sums = sums + jnp.dot(lhs[:, 512:768], tabs[c, 0:256, :], preferred_element_type=F32)
                cols = pl.ds(pl.multiple_of(128 * c, 128), 128)
                tre, tim = base_re[40:48, cols], base_im[40:48, cols]
                xr, xi = sums[0:32, 0:128], sums[0:32, 128:256]
                for h in range(1, 8):
                    gr, gi = sums[32 * h : 32 * h + 32, 0:128], sums[32 * h : 32 * h + 32, 128:256]
                    cr, ci = tre[h : h + 1], tim[h : h + 1]
                    xr = xr + gr * cr + gi * ci
                    xi = xi + gi * cr - gr * ci
                parts = [x[8 * v : 8 * v + 8] for v in range(4) for x in (xr, xi)]
                for i, block in enumerate(swap_blocks(parts, lane)):
                    send2[i % 2, 4 * c + i // 2, b] = block
            for k in range(2):
                c = 2 * lax.rem(g // 8 + far_first(step), 4) + lax.rem(level + 1 + k, 2)
                for d in range(4):
                    owner = 4 * c + lax.rem(g + d, 4)
                    if k == 1 and d == 0:

                        @pl.when(step < 3)
                        def _():
                            start2(b, owner)

                    else:
                        start2(b, owner)

            @pl.when(step == 3)
            def _():
                start2_own(b)

            return carry

        lax.fori_loop(0, 4, chunk, 0)

    each_peer(g, lambda owner: start2(2, owner))
    start2_own(2)

    loads[2].wait()

    def copy3(hf, p, src, peer):
        return pltpu.make_async_remote_copy(
            src_ref=send3.at[hf, src, p], dst_ref=out_ref.at[p, my_level, pl.ds(16 * hf, 16)],
            send_sem=s3.at[hf], recv_sem=r3.at[hf], device_id=(g, peer), device_id_type=MESH,
        )

    def own(hf):
        return pltpu.make_async_copy(send3.at[hf, z], out_ref.at[:, my_level, pl.ds(16 * hf, 16)], own_sem.at[hf])

    for hf in range(2):
        for b in range(2):

            if hf == 0 or b == 0:
                each_size(lambda count: all2(2 * hf + b, count).wait_recv())
            hi, lo = split(recv2[hf, :, b].reshape(256, 128).T)
            both = jnp.concatenate([hi, hi, lo], axis=1)
            ybuf[pl.ds(128 * b, 128), :] = jnp.dot(both, w_ref[...], preferred_element_type=F32)

        def finish(tile, carry):
            at = pl.multiple_of(8 * tile, 8)
            values = []
            for v in range(8):
                rr = ybuf[pl.ds(32 * v + at, 8), :]
                ii = ybuf[pl.ds(32 * v + 16 + at, 8), :]
                re = rr[:, :256] - ii[:, 256:]
                im = rr[:, 256:] + ii[:, :256]
                c, s = twiddle_ref[v : v + 1, :], twiddle_ref[8 + v : 9 + v, :]
                values.append((re * c + im * s, im * c - re * s))
            for q, (re, im) in enumerate(eight_points(values)):
                send3[hf, q, 0, pl.ds(at, 8), :] = re
                send3[hf, q, 1, pl.ds(at, 8), :] = im
            return carry

        lax.fori_loop(0, 2, finish, 0)
        own(hf).start()
        for d in FAR_FIRST:
            peer = lax.rem(z + d, GY)
            for p in range(2):
                copy3(hf, p, peer, peer).start()

    for b in range(2):
        all1(b).wait_send()
    for part in range(3):
        each_size(lambda count: all2(part, count).wait_send())
    for hf in range(2):
        own(hf).wait()
        arrived = out_ref.at[:, pl.ds(0, GY - 1), pl.ds(16 * hf, 16)]
        both = group(send3.at[hf, pl.ds(0, GY - 1)], arrived, s3.at[hf], r3.at[hf])
        both.wait_recv()
        both.wait_send()


def y_tables():
    turns = np.outer(np.arange(256), np.arange(256)) % 256 * (2.0 * np.pi / 256)
    table = np.concatenate([np.cos(turns), -np.sin(turns)], axis=1).astype(np.float32)
    high = table.astype(jnp.bfloat16)
    low = (table - high.astype(np.float32)).astype(jnp.bfloat16)
    return np.concatenate([high, low, high], axis=0)


def shards(fields, wave_order, kept_mask):
    w = y_tables()
    dma = pltpu.SemaphoreType.DMA
    result = pl.pallas_call(
        kernel,
        out_shape=jax.ShapeDtypeStruct((2, 8, 32, 256), F32),
        in_specs=[pl.BlockSpec(memory_space=pltpu.HBM)] * 3,
        out_specs=pl.BlockSpec(memory_space=pltpu.HBM),
        scratch_shapes=[
            pltpu.VMEM((8, 64, 256), F32),
            pltpu.VMEM((1, 1024), jnp.int32),
            pltpu.VMEM((768, 512), BF16),
            pltpu.VMEM((16, 256), F32),
            dma((3,)),
            pltpu.VMEM((2, 32, 8, 256), F32),
            pltpu.VMEM((2, 32, 8, 256), F32),
            pltpu.VMEM((48, 1024), F32),
            pltpu.VMEM((48, 1024), F32),
            pltpu.VMEM((8, 512, 256), BF16),
            pltpu.VMEM((256, 768), BF16),
            pltpu.VMEM((2, 32, 2, 8, 128), F32),
            pltpu.VMEM((2, 32, 2, 8, 128), F32),
            pltpu.VMEM((256, 512), F32),
            pltpu.VMEM((2, 8, 2, 16, 256), F32),
            pltpu.VMEM((2, 8, 2, 16, 256), F32),
            dma((2,)), dma((2,)), dma((3,)), dma((3,)), dma((2,)), dma((2,)), dma((2,)),
        ],
        compiler_params=pltpu.CompilerParams(has_side_effects=True, collective_id=0, vmem_limit_bytes=int(67043328-10.75*1048576)),
        name="bifourier",
    )(fields, wave_order.reshape(1, 1024), jnp.asarray(w))
    bound = (result != result).astype(jnp.int32)
    return jnp.where(kept_mask[None, None] > bound, result, 0.0)


def solution(mesh):
    return jax.shard_map(
        shards,
        mesh=mesh,
        in_specs=(P(None, "gx", "gy"), P(), P("gx", "gy")),
        out_specs=P(None, None, "gx", "gy"),
        check_vma=False,
    )
```
